32 devices in a mesh: dp: 32 (over z, y, x, core).
Axes of the slice: x: 2, y: 2, z: 4, core: 2. Of those that a mesh axis runs over, the one named last changes fastest.
Arguments:
- grad_embed: bfloat16 [32, 4000, 2304], P('dp')
- grad_q: bfloat16 [32, 6, 2304, 32], P('dp')
- grad_k: bfloat16 [32, 6, 2304, 16], P('dp')
- grad_v: bfloat16 [32, 6, 2304, 16], P('dp')
- grad_out: bfloat16 [32, 6, 32, 2304], P('dp')
- grad_gate: bfloat16 [32, 6, 2304, 144], P('dp')
- grad_up: bfloat16 [32, 6, 2304, 144], P('dp')
- grad_down: bfloat16 [32, 6, 144, 2304], P('dp')
- grad_norms: bfloat16 [32, 6, 4, 2304], P('dp')
- grad_qk_norms: bfloat16 [32, 6, 2, 256], P('dp')
- first_moment: float32 [16573440], P('dp')
- second_moment: float32 [16573440], P('dp')
- master_param: float32 [16573440], P('dp')
- hyper_params: float32 [5], replicated
Outputs:
- output 1: bfloat16 [4000, 2304], replicated
- output 2: bfloat16 [6, 2304, 32], replicated
- output 3: bfloat16 [6, 2304, 16], replicated
- output 4: bfloat16 [6, 2304, 16], replicated
- output 5: bfloat16 [6, 32, 2304], replicated
- output 6: bfloat16 [6, 2304, 144], replicated
- output 7: bfloat16 [6, 2304, 144], replicated
- output 8: bfloat16 [6, 144, 2304], replicated
- output 9: bfloat16 [6, 4, 2304], replicated
- output 10: bfloat16 [6, 2, 256], replicated
- output 11: float32 [16573440], P('dp')
- output 12: float32 [16573440], P('dp')
- output 13: float32 [16573440], P('dp')
All inputs are finite; a program needn't handle non-finite values.
Results may differ from the reference program's by a relative error of at most 0.001.
Values are sent between devices in bfloat16 or wider.
A program may use at most 1 GiB of HBM per device.

```python
import math
import jax
import jax.numpy as jnp

D_MODEL = 2304
FF_WIDTH = 9216
Q_HEADS = 8
KV_HEADS = 4
HEAD_DIM = 256
VOCAB_SIZE = 256000
TP_RANKS = 64
NUM_LAYERS = 6
DATA_PAR = 32
ADAM_STEP = 7

ADAM_EPS = 1e-8
CLIP_EPS = 1e-6
Q_COLS = Q_HEADS * HEAD_DIM // TP_RANKS
KV_COLS = KV_HEADS * HEAD_DIM // TP_RANKS
FF_COLS = FF_WIDTH // TP_RANKS
VOCAB_ROWS = VOCAB_SIZE // TP_RANKS
PARAM_SHAPES = ((VOCAB_ROWS, D_MODEL), (NUM_LAYERS, D_MODEL, Q_COLS), (NUM_LAYERS, D_MODEL, KV_COLS), (NUM_LAYERS, D_MODEL, KV_COLS), (NUM_LAYERS, Q_COLS, D_MODEL), (NUM_LAYERS, D_MODEL, FF_COLS), (NUM_LAYERS, D_MODEL, FF_COLS), (NUM_LAYERS, FF_COLS, D_MODEL), (NUM_LAYERS, 4, D_MODEL), (NUM_LAYERS, 2, HEAD_DIM))
PARAM_SIZES = tuple(math.prod(tensor_dims) for tensor_dims in PARAM_SHAPES)
PARAMS_TOTAL = sum(PARAM_SIZES)
DECAY_LEN = PARAMS_TOTAL - PARAM_SIZES[8] - PARAM_SIZES[9]
GRAD_NAMES = ("grad_embed", "grad_q", "grad_k", "grad_v", "grad_out", "grad_gate", "grad_up", "grad_down", "grad_norms", "grad_qk_norms")


def setup_inputs(seed: int = 0) -> dict:
    key_list = jax.random.split(jax.random.key(seed), 16)
    grad_scale = math.sqrt(DATA_PAR)
    inputs = {}
    square_sum = jnp.float32(0.0)
    for tensor_index, tensor_dims in enumerate(PARAM_SHAPES):
        noise_draw = jax.random.normal(key_list[tensor_index], (DATA_PAR,) + tensor_dims, jnp.float32)
        grad_arr = (grad_scale * noise_draw).astype(jnp.bfloat16)
        mean_grad = jnp.sum(grad_arr, axis=0, dtype=jnp.float32) / DATA_PAR
        square_sum = square_sum + jnp.sum(mean_grad * mean_grad)
        inputs[GRAD_NAMES[tensor_index]] = grad_arr
    inputs["first_moment"] = 0.1 * jax.random.normal(key_list[10], (PARAMS_TOTAL,), jnp.float32)
    inputs["second_moment"] = 0.015 * jnp.exp(0.5 * jax.random.normal(key_list[11], (PARAMS_TOTAL,), jnp.float32))
    inputs["master_param"] = 0.5 * jax.random.normal(key_list[12], (PARAMS_TOTAL,), jnp.float32)
    hyper_draw = jax.random.uniform(key_list[13], (5,), jnp.float32)
    inputs["hyper_params"] = jnp.stack([0.05 + 0.1 * hyper_draw[0], 0.8 + 0.15 * hyper_draw[1], 0.9 + 0.09 * hyper_draw[2], 0.3 + 1.2 * hyper_draw[3], (0.3 + 0.4 * hyper_draw[4]) * jnp.sqrt(square_sum)])
    return inputs


def reference(grad_embed, grad_q, grad_k, grad_v, grad_out, grad_gate, grad_up, grad_down, grad_norms, grad_qk_norms, first_moment, second_moment, master_param, hyper_params):
    grads = (grad_embed, grad_q, grad_k, grad_v, grad_out, grad_gate, grad_up, grad_down, grad_norms, grad_qk_norms)
    mean_grad = jnp.concatenate([jnp.sum(grad_arr, axis=0, dtype=jnp.float32).reshape(-1) for grad_arr in grads]) / DATA_PAR
    learn_rate = hyper_params[0]
    beta_one = hyper_params[1]
    beta_two = hyper_params[2]
    weight_decay = hyper_params[3]
    grad_norm = jnp.sqrt(jnp.sum(mean_grad * mean_grad))
    clip_scale = jnp.minimum(1.0, hyper_params[4] / (grad_norm + CLIP_EPS))
    clipped = mean_grad * clip_scale
    moment_one = beta_one * first_moment + (1.0 - beta_one) * clipped
    moment_two = beta_two * second_moment + (1.0 - beta_two) * (clipped * clipped)
    m_hat = moment_one / (1.0 - beta_one ** ADAM_STEP)
    v_hat = moment_two / (1.0 - beta_two ** ADAM_STEP)
    keep_decay = jnp.arange(PARAMS_TOTAL) < DECAY_LEN
    direction = m_hat / (jnp.sqrt(v_hat) + ADAM_EPS) + jnp.where(keep_decay, weight_decay * master_param, 0.0)
    new_master = master_param - learn_rate * direction
    new_params = new_master.astype(jnp.bfloat16)
    out_list = []
    start_pos = 0
    for tensor_dims, tensor_size in zip(PARAM_SHAPES, PARAM_SIZES):
        out_list.append(new_params[start_pos:start_pos + tensor_size].reshape(tensor_dims))
        start_pos = start_pos + tensor_size
    return (out_list[0], out_list[1], out_list[2], out_list[3], out_list[4], out_list[5], out_list[6], out_list[7], out_list[8], out_list[9], moment_one, moment_two, new_master)
```

```python
import math
import jax
import jax.numpy as jnp
from jax import lax
from jax.sharding import PartitionSpec as P
from jax.experimental import pallas as pl
from jax.experimental.pallas import tpu as pltpu

ADAM_STEP = 7
ADAM_EPS = 1e-8
CLIP_EPS = 1e-6

SUB, LANES = 8, 128
TILES = 18
HALF = TILES // 2
ROWS = TILES * SUB
UNIT = ROWS * LANES
WIDTH = TILES * LANES
LAYERS = 6
DEVICES = 32
SHARD = 517920
NORM_LEN = 58368
TAIL = (TILES, SUB, LANES)
STARTS = (0, 500, 524, 536, 548, 572, 680, 788, 896, 900)
EMBED, Q, K, V, OUT, GATE, UP, DOWN, NORMS, END = STARTS
TENSORS = len(STARTS) - 1
COVER = 30
GATHER = 29
HALO = 2 * ROWS
OWN_ROWS = 4048
OWN_BLOCK = 176
FLAT_ROWS = COVER * ROWS
LINE = 4
SHIFTED = {17: 476, 18: 504}


def first_units():
    firsts = [SHIFTED.get(r, (r * SHARD) // UNIT) for r in range(DEVICES)]
    return firsts + [END]


FIRST = first_units()
COVER_FIRST = [min(first, END - COVER) for first in FIRST]
ANY = pl.BlockSpec(memory_space=pl.ANY)
IN_VMEM = pl.BlockSpec(memory_space=pltpu.VMEM)
IN_SMEM = pl.BlockSpec(memory_space=pltpu.SMEM)
BIG_VMEM = 66_000_000


def first_unit(r):
    value = r * (SHARD // math.gcd(SHARD, UNIT)) // (UNIT // math.gcd(SHARD, UNIT))
    for device, first in SHIFTED.items():
        value = jnp.where(r == device, first, value)
    return jnp.where(r == DEVICES, END, value)


def unit_runs(start, stop):
    runs = []
    for tensor in range(TENSORS):
        low, high = max(start, STARTS[tensor]), min(stop, STARTS[tensor + 1])
        if low < high:
            runs.append((tensor, low - STARTS[tensor], high - low, low - start))
    return runs


def tile_copies(refs, runs, slot_ref):
    pairs = []
    for tensor, first, count, slot in runs:
        ref = refs[tensor]
        kind = STARTS[tensor]
        if kind in (EMBED, OUT, DOWN, NORMS):
            pairs.append((ref.at[pl.ds(first, count)], slot_ref.at[pl.ds(slot, count)]))
        elif kind in (GATE, UP):
            for k in range(count):
                layer, col = divmod(first + k, TILES)
                pairs.append((ref.at[layer, :, col], slot_ref.at[slot + k]))
        else:
            step = 2 if kind == Q else 1
            for k in range(0, count, step):
                layer, half = divmod((first + k) // step, 2)
                for row in range(2 * step):
                    part = slot_ref.at[slot + k + row // 2, pl.ds(HALF * (row % 2), HALF)]
                    pairs.append((ref.at[layer, row, pl.ds(HALF * half, HALF)], part))
    return pairs

SLOTS = 8


def pack_kernel(*args):
    refs, (out_ref, stage, in_sem, out_sem) = args[:TENSORS], args[TENSORS:]
    depth = stage.shape[0]

    def start_in(r):
        slot = r % depth
        if r >= depth:
            pltpu.make_async_copy(stage.at[slot], out_ref.at[r - depth], out_sem.at[slot]).wait()
        for src, dst in tile_copies(refs, unit_runs(COVER_FIRST[r], COVER_FIRST[r] + COVER), stage.at[slot]):
            pltpu.make_async_copy(src, dst, in_sem.at[slot]).start()

    ahead = depth // 2
    for r in range(ahead):
        start_in(r)
    for r in range(DEVICES):
        if r + ahead < DEVICES:
            start_in(r + ahead)
        slot = r % depth
        pltpu.make_async_copy(out_ref.at[r], stage.at[slot], in_sem.at[slot]).wait()
        pltpu.make_async_copy(stage.at[slot], out_ref.at[r], out_sem.at[slot]).start()
    for r in range(DEVICES - depth, DEVICES):
        slot = r % depth
        pltpu.make_async_copy(stage.at[slot], out_ref.at[r], out_sem.at[slot]).wait()


def pack(tensors):
    return pl.pallas_call(
        pack_kernel,
        name="pack",
        out_shape=jax.ShapeDtypeStruct((DEVICES, COVER) + TAIL, jnp.bfloat16),
        in_specs=[ANY] * TENSORS,
        out_specs=ANY,
        scratch_shapes=[
            pltpu.VMEM((SLOTS, COVER) + TAIL, jnp.bfloat16),
            pltpu.SemaphoreType.DMA((SLOTS,)),
            pltpu.SemaphoreType.DMA((SLOTS,)),
        ],
        compiler_params=pltpu.CompilerParams(vmem_limit_bytes=BIG_VMEM),
    )(*tensors)


def unpack_kernel(*args):
    gathered, outs, (stage, in_sem, out_sem) = args[0], args[1:-3], args[-3:]
    depth = stage.shape[0]

    def wait_out(r):
        slot = r % depth
        count = FIRST[r + 1] - FIRST[r]
        part = stage.at[slot, pl.ds(0, count)]
        pltpu.make_async_copy(part, gathered.at[r, pl.ds(0, count)], out_sem.at[slot]).wait()

    def start_in(r):
        slot = r % depth
        if r >= depth:
            wait_out(r - depth)
        pltpu.make_async_copy(gathered.at[r], stage.at[slot], in_sem.at[slot]).start()

    ahead = depth // 2
    for r in range(ahead):
        start_in(r)
    for r in range(DEVICES):
        if r + ahead < DEVICES:
            start_in(r + ahead)
        slot = r % depth
        pltpu.make_async_copy(gathered.at[r], stage.at[slot], in_sem.at[slot]).wait()
        for dst, src in tile_copies(outs, unit_runs(FIRST[r], FIRST[r + 1]), stage.at[slot]):
            pltpu.make_async_copy(src, dst, out_sem.at[slot]).start()
    for r in range(DEVICES - depth, DEVICES):
        wait_out(r)


def unpack(gathered, tensor_shapes):
    return pl.pallas_call(
        unpack_kernel,
        name="unpack",
        out_shape=[jax.ShapeDtypeStruct(dims, jnp.bfloat16) for dims in tensor_shapes],
        in_specs=[ANY],
        out_specs=[ANY] * TENSORS,
        scratch_shapes=[
            pltpu.VMEM((SLOTS, GATHER) + TAIL, jnp.bfloat16),
            pltpu.SemaphoreType.DMA((SLOTS,)),
            pltpu.SemaphoreType.DMA((SLOTS,)),
        ],
        compiler_params=pltpu.CompilerParams(vmem_limit_bytes=BIG_VMEM),
    )(gathered)


def place():
    me = lax.axis_index("dp")
    return me // 8, (me // 4) % 2, (me // 2) % 2, me % 2


def index_of(z, y, x, c):
    return ((z * 2 + y) * 2 + x) * 2 + c


def greet(peers):
    barrier = pltpu.get_barrier_semaphore()
    for peer in peers:
        pl.semaphore_signal(barrier, inc=1, device_id=(peer,), device_id_type=pl.DeviceIdType.MESH)
    pl.semaphore_wait(barrier, len(peers))


def remote(src, dst, send, recv, peer):
    return pltpu.make_async_remote_copy(src_ref=src, dst_ref=dst, send_sem=send, recv_sem=recv, device_id=(peer,), device_id_type=pl.DeviceIdType.MESH)


class Sems:
    def __init__(self, send, recv):
        self.send, self.recv, self.used = send, recv, 0

    def copy(self, src, dst, peer):
        k = self.used
        self.used += 1
        return remote(src, dst, self.send.at[k], self.recv.at[k], peer)


COLORS = range(4)
OUTER = 7


def jobs_of(sizes, first=0):
    steps = [[] for _ in sizes[0]]
    for color in COLORS:
        for step, count in enumerate(sizes[color]):
            if count:
                steps[step].append((color, first, count))
                first += count
    return steps


RS_WIDE, RS_THIN = (1,) * 10, (1, 0) * 5
RS_STEPS = jobs_of((RS_WIDE, RS_WIDE, RS_THIN, RS_THIN))


class Reduce:
    def __init__(self, job, x_ref, g_ref, own, sum1, own_sem, sum_slot, got1, got2, got3, send, recv):
        self.color, self.first, self.count = job
        self.units = pl.ds(self.first, self.count)
        self.g_ref = g_ref
        z, y, x, c = place()
        self.z = z
        self.late = self.color >= 2
        by_x = self.color % 2 == 0
        self.mine = y if by_x else x
        if by_x:
            group = ((y, 1 - x, c), (y, 1 - x, 1 - c), (y, x, 1 - c))
            side = index_of(z, 1 - y, x, c)
            part = lambda yy, xx, cc: x_ref.at[:, :, xx, cc, self.units]
        else:
            group = ((1 - y, x, c), (1 - y, x, 1 - c), (y, x, 1 - c))
            side = index_of(z, y, 1 - x, c)
            part = lambda yy, xx, cc: x_ref.at[:, yy, :, cc, self.units]
        n = pl.ds(0, self.count)
        self.own = own.at[sum_slot, self.color, :, :, n]
        self.sum1 = sum1.at[sum_slot, self.color, :, :, n]
        self.got1, self.got2, self.got3 = got1, got2, got3
        sems = Sems(send, recv)
        self.copies1 = [sems.copy(part(*who), got1.at[k], index_of(z, *who)) for k, who in enumerate(group)]
        self.own_copy = pltpu.make_async_copy(part(y, x, c), self.own, own_sem.at[sum_slot, self.color])
        others = [(z + k) % LINE for k in range(1, LINE)]
        peers = [index_of(zz, y, x, c) for zz in others]
        if self.late:
            self.copies2 = [sems.copy(self.sum1.at[zz], got2.at[k], peer) for k, (zz, peer) in enumerate(zip(others, peers))]
            self.copies3 = [sems.copy(got2.at[0, 1 - self.mine], got3.at[0], side)]
        else:
            self.copies2 = [sems.copy(self.sum1.at[:, 1 - self.mine], got2, side)]
            self.copies3 = [sems.copy(got2.at[zz], got3.at[k], peer) for k, (zz, peer) in enumerate(zip(others, peers))]

    def add1(self):
        def body(i, carry):
            zz, side, u = i // (2 * self.count), (i // self.count) % 2, i % self.count
            total = self.own[zz, side, u].astype(jnp.float32)
            for k in range(len(self.copies1)):
                total = total + self.got1[k, zz, side, u].astype(jnp.float32)
            self.sum1[zz, side, u] = total
            return carry

        lax.fori_loop(0, 2 * LINE * self.count, body, 0)

    def add2(self):
        def early(i, carry):
            zz, u = i // self.count, i % self.count
            self.got2[zz, u] = self.got2[zz, u] + self.sum1[zz, self.mine, u]
            return carry

        def late(i, carry):
            side, u = i // self.count, i % self.count
            total = self.sum1[self.z, side, u]
            for k in range(LINE - 1):
                total = total + self.got2[k, side, u]
            self.got2[0, side, u] = total
            return carry

        if self.late:
            lax.fori_loop(0, 2 * self.count, late, 0)
        else:
            lax.fori_loop(0, LINE * self.count, early, 0)

    def add3(self, begin, end, acc):
        def body(u, acc):
            total = self.got2[0, self.mine, u] if self.late else self.got2[self.z, u]
            for k in range(len(self.copies3)):
                total = total + self.got3[k, u]
            mean = total * (1.0 / DEVICES)
            slot = self.first + u
            self.g_ref[slot] = mean
            square = jnp.sum(mean * mean, axis=0)
            return acc + jnp.where((slot >= begin) & (slot < end), square, 0.0)

        return lax.fori_loop(0, self.count, body, acc)


def start_all(copies):
    for copy in copies:
        copy.start()


def recv_all(copies):
    for copy in copies:
        copy.wait_recv()


def send_all(copies):
    for copy in copies:
        copy.wait_send()


def reduce_kernel(*args):
    x_ref, g_ref, n_ref, own, sum1, norm_buf, own_sem, send_n, recv_n = args[:9]
    rest = list(args[9:])
    z, y, x, c = place()
    me = lax.axis_index("dp")
    z_peers = [index_of((z + k) % LINE, y, x, c) for k in range(1, LINE)]
    plane = [index_of(z, y, x, 1 - c), index_of(z, y, 1 - x, c), index_of(z, y, 1 - x, 1 - c), index_of(z, 1 - y, x, c), index_of(z, 1 - y, x, 1 - c)]
    greet(plane + z_peers)
    steps = []
    for t, jobs in enumerate(RS_STEPS):
        steps.append([])
        for job in jobs:
            steps[t].append(Reduce(job, x_ref, g_ref, own, sum1, own_sem, t % 2, *rest[:5]))
            rest = rest[5:]
    total_steps = len(steps)

    def start1(t):
        for k in range(3):
            for job in steps[t]:
                job.copies1[k].start()
        for job in steps[t]:
            job.own_copy.start()

    first = first_unit(me)
    begin = first - jnp.minimum(first, END - COVER)
    end = begin + first_unit(me + 1) - first
    acc = jnp.zeros((SUB, LANES), jnp.float32)
    start1(0)
    for t in range(total_steps + 2):
        if t + 1 < total_steps:
            start1(t + 1)
        if t < total_steps:
            for job in steps[t]:
                recv_all(job.copies1)
                job.own_copy.wait()
                if t >= 2:
                    send_all([copy for old in steps[t - 2] if old.color == job.color for copy in old.copies2])
                job.add1()
            for job in steps[t]:
                start_all(job.copies2)
        if 1 <= t <= total_steps:
            for job in steps[t - 1]:
                recv_all(job.copies2)
                job.add2()
            for job in steps[t - 1]:
                start_all(job.copies3)
        if t >= 2:
            for job in steps[t - 2]:
                recv_all(job.copies3)
                acc = job.add3(begin, end, acc)

    sems = Sems(send_n, recv_n)
    sent, used = [], 0
    norm_buf[0] = acc
    for peers in (z_peers, plane[:3], plane[3:4]):
        copies = [sems.copy(norm_buf.at[used], norm_buf.at[used + 1 + k], peer) for k, peer in enumerate(peers)]
        start_all(copies)
        recv_all(copies)
        sent += copies
        total = norm_buf[used]
        for k in range(len(peers)):
            total = total + norm_buf[used + 1 + k]
        used += 1 + len(peers)
        norm_buf[used] = total
    n_ref[0] = jnp.sum(norm_buf[used])

    send_all(sent)
    for t, jobs in enumerate(steps):
        for job in jobs:
            send_all(job.copies1 + job.copies3)
            if not any(later.color == job.color for later in sum(steps[t + 2:t + 3], [])):
                send_all(job.copies2)


def reduce_scatter(packed):
    dma = pltpu.SemaphoreType.DMA
    scratch = []
    largest = max(RS_WIDE)
    for color, first, count in sum(RS_STEPS, []):
        late = color >= 2
        scratch += [
            pltpu.VMEM((3, LINE, 2, count) + TAIL, jnp.bfloat16),
            pltpu.VMEM(((3, 2, count) if late else (LINE, count)) + TAIL, jnp.float32),
            pltpu.VMEM((1 if late else 3, count) + TAIL, jnp.float32),
            dma((OUTER,)),
            dma((OUTER,)),
        ]
    return pl.pallas_call(
        reduce_kernel,
        name="reduce_scatter",
        out_shape=[jax.ShapeDtypeStruct((COVER,) + TAIL, jnp.float32), jax.ShapeDtypeStruct((1,), jnp.float32)],
        in_specs=[ANY],
        out_specs=[IN_VMEM, IN_SMEM],
        scratch_shapes=[
            pltpu.VMEM((2, len(COLORS), LINE, 2, largest) + TAIL, jnp.bfloat16),
            pltpu.VMEM((2, len(COLORS), LINE, 2, largest) + TAIL, jnp.float32),
            pltpu.VMEM((11, SUB, LANES), jnp.float32),
            dma((2, len(COLORS))),
            dma((OUTER,)),
            dma((OUTER,)),
        ] + scratch,
        compiler_params=pltpu.CompilerParams(collective_id=0, has_side_effects=True, vmem_limit_bytes=BIG_VMEM),
    )(packed.reshape((LINE, 2, 2, 2, COVER) + TAIL))


AG_STEPS = jobs_of(((1,) * 10, (1,) * 9 + (0,), (1, 0) * 5, (1, 0) * 5))


class Gather:
    def __init__(self, job, a_ref, b_ref, send, recv):
        color, first, count = job
        u = pl.ds(first, count)
        z, y, x, c = place()
        z_peers = [index_of((z + k) % LINE, y, x, c) for k in range(1, LINE)]
        y_peer, x_peer, c_peer = index_of(z, 1 - y, x, c), index_of(z, y, 1 - x, c), index_of(z, y, x, 1 - c)
        by_x = color % 2 == 0
        side, last = (y_peer, x_peer) if by_x else (x_peer, y_peer)
        sems = Sems(send, recv)
        here, row = b_ref.at[z, y, x, c, u], b_ref.at[:, y, x, c, u]
        pair = b_ref.at[z, :, x, c, u] if by_x else b_ref.at[z, y, :, c, u]
        half = b_ref.at[:, :, x, c, u] if by_x else b_ref.at[:, y, :, c, u]
        full = b_ref.at[:, :, :, c, u]
        if color < 2:
            self.stages = [[sems.copy(a_ref.at[u], here, peer) for peer in z_peers], [sems.copy(row, row, side)]]
        else:
            self.stages = [[sems.copy(a_ref.at[u], here, side)], [sems.copy(pair, pair, peer) for peer in z_peers]]
        self.stages += [[sems.copy(half, half, last)], [sems.copy(full, full, c_peer)]]


def gather_kernel(a_ref, b_ref, own_sem, *rest):
    z, y, x, c = place()
    z_peers = [index_of((z + k) % LINE, y, x, c) for k in range(1, LINE)]
    greet(z_peers + [index_of(z, 1 - y, x, c), index_of(z, y, 1 - x, c), index_of(z, y, x, 1 - c)])
    own = pltpu.make_async_copy(a_ref.at[pl.ds(0, GATHER)], b_ref.at[z, y, x, c], own_sem)
    own.start()
    steps = []
    for jobs in AG_STEPS:
        steps.append([])
        for job in jobs:
            steps[-1].append(Gather(job, a_ref, b_ref, *rest[:2]))
            rest = rest[2:]
    count, stages = len(steps), 4

    def start(t, stage):
        if 0 <= t < count:
            if stage:
                for job in steps[t]:
                    recv_all(job.stages[stage - 1])
                    start_all(job.stages[stage])
            else:
                for job in steps[t]:
                    start_all(job.stages[0])

    start(0, 0)
    start(1, 0)
    own.wait()
    for t in range(count + stages):
        start(t + 2, 0)
        for stage in range(1, stages):
            start(t + 1 - stage, stage)
    for jobs in steps:
        for job in jobs:
            recv_all(job.stages[-1])
            for copies in job.stages:
                send_all(copies)


def all_gather(chunk):
    dma = pltpu.SemaphoreType.DMA
    out = pl.pallas_call(
        gather_kernel,
        name="all_gather",
        out_shape=jax.ShapeDtypeStruct((LINE, 2, 2, 2, GATHER) + TAIL, jnp.bfloat16),
        in_specs=[IN_VMEM],
        out_specs=ANY,
        scratch_shapes=[dma] + [dma((OUTER,))] * (2 * len(sum(AG_STEPS, []))),
        compiler_params=pltpu.CompilerParams(collective_id=1, has_side_effects=True, vmem_limit_bytes=BIG_VMEM),
    )(chunk)
    return out.reshape((DEVICES, GATHER) + TAIL)


def lanes(rows):
    return lax.broadcasted_iota(jnp.int32, (rows, LANES), 1)


def among(u, *starts):
    found = False
    for start in starts:
        stop = STARTS[STARTS.index(start) + 1]
        found = ((u >= start) & (u < stop)) | found
    return found


def rolled(value, shift):
    shift = shift % LANES
    return value if shift == 0 else pltpu.roll(value, shift, 1)


def turned(tiles):
    blank = [jnp.zeros((SUB, LANES), jnp.float32)] * (LANES // SUB - len(tiles))
    return jnp.concatenate(tiles + blank, axis=0).T


def narrow_blocks(width):
    step = LANES // width
    return [(col, min(step, HALF - col)) for col in range(0, HALF, step)]


def tile(ref, unit, index):
    return ref.at[pl.ds(pl.multiple_of(unit * ROWS + index * SUB, SUB), SUB), :]


def narrow_to_flat(in_ref, unit, flat, row, wide, width):
    per, step, lane = width // SUB, LANES // width, lanes(width)
    for col, count in narrow_blocks(width):
        wide[...] = turned([tile(in_ref, unit, HALF * r + col + e)[...] for e in range(count) for r in range(per)])
        for e in range(count):
            value = None
            for j in range(step):
                pick = rolled(wide[pl.ds(j, width, stride=step), :], width * (j - e))
                value = pick if value is None else jnp.where(lane >= width * j, pick, value)
            flat[pl.ds(row + width * (col + e), width), :] = value


def narrow_to_tiles(flat, row, out_ref, unit, wide, width):
    per, step, lane = width // SUB, LANES // width, lanes(width)
    for col, count in narrow_blocks(width):
        for j in range(step):
            value = None
            for e in range(count):
                pick = rolled(flat[pl.ds(row + width * (col + e), width), :], width * (e - j))
                value = pick if value is None else jnp.where(lane >= width * e, pick, value)
            wide[pl.ds(j, width, stride=step), :] = value
        back = wide[...].T
        for e in range(count):
            for r in range(per):
                at = width * e + SUB * r
                index = HALF * r + col + e
                out_ref[unit + index // TILES, index % TILES] = back[at:at + SUB].astype(jnp.bfloat16)


EDGE = ROWS - LANES


def unit_to_flat(in_ref, unit, flat, row, u, wide, tail):
    @pl.when(among(u, EMBED, OUT, DOWN))
    def _():
        for e in range(SUB):
            flat[pl.ds(row + TILES * e, TILES), :] = in_ref[pl.ds(row + e, TILES, stride=SUB), :]

    @pl.when(among(u, NORMS))
    def _():
        flat[pl.ds(row, ROWS), :] = in_ref[pl.ds(row, ROWS), :]

    @pl.when(among(u, K, V))
    def _():
        narrow_to_flat(in_ref, unit, flat, row, wide, EDGE)

    @pl.when(among(u, GATE, UP))
    def _():
        wide[...] = turned([tile(in_ref, unit, t)[...] for t in range(LANES // SUB)])
        tail[...] = turned([tile(in_ref, unit, t)[...] for t in range(LANES // SUB, TILES)])
        lane = lanes(EDGE)
        before = None
        for j in range(SUB):
            head = rolled(wide[pl.ds(j, EDGE, stride=SUB), :], EDGE * j)
            rest = rolled(tail[pl.ds(j, EDGE, stride=SUB), :], EDGE * j)
            flat[pl.ds(row + j, EDGE, stride=HALF), :] = head if before is None else jnp.where(lane < EDGE * j, before, head)
            before = jnp.where((lane >= EDGE * j) & (lane < EDGE * (j + 1)), rest, head)
        flat[pl.ds(row + SUB, EDGE, stride=HALF), :] = before


def unit_to_tiles(flat, row, out_ref, unit, u, wide, tail):
    @pl.when(among(u, EMBED, OUT, DOWN))
    def _():
        for t in range(TILES):
            out_ref[unit, t] = flat[pl.ds(row + t, SUB, stride=TILES), :].astype(jnp.bfloat16)

    @pl.when(among(u, NORMS))
    def _():
        out_ref[unit] = flat[pl.ds(row, ROWS), :].reshape(TAIL).astype(jnp.bfloat16)

    @pl.when(among(u, K, V))
    def _():
        narrow_to_tiles(flat, row, out_ref, unit, wide, EDGE)

    @pl.when(among(u, GATE, UP))
    def _():
        lane = lanes(EDGE)
        for j in range(SUB):
            here = flat[pl.ds(row + j, EDGE, stride=HALF), :]
            after = flat[pl.ds(row + j + 1, EDGE, stride=HALF), :]
            wide[pl.ds(j, EDGE, stride=SUB), :] = rolled(jnp.where(lane >= EDGE * j, here, after), -EDGE * j)
            tail[pl.ds(j, EDGE, stride=SUB), :] = rolled(after, -EDGE * j)
        out_ref[unit, pl.ds(0, LANES // SUB)] = wide[...].T.reshape(LANES // SUB, SUB, LANES).astype(jnp.bfloat16)
        out_ref[unit, pl.ds(LANES // SUB, 2)] = tail[...].T[0:EDGE].reshape(2, SUB, LANES).astype(jnp.bfloat16)


def local_place():
    me = lax.axis_index("dp")
    return me, first_unit(me)


def blocks_of(rows, block, body):
    def step(i, carry):
        body(pl.multiple_of(i * block, SUB))
        return carry

    lax.fori_loop(0, rows // block, step, 0)


def to_flat_kernel(in_ref, out_ref, flat, wide, tail):
    me, first = local_place()
    first = jnp.minimum(first, END - COVER)
    offset = me * SHARD - first * UNIT

    def pair(i, carry):
        unit = 2 * i
        u = first + unit

        @pl.when(among(u, Q))
        def _():
            narrow_to_flat(in_ref, unit, flat, unit * ROWS, wide, 2 * EDGE)

        for j in range(2):
            unit_to_flat(in_ref, unit + j, flat, (unit + j) * ROWS, u + j, wide, tail)
        return carry

    lax.fori_loop(0, COVER // 2, pair, 0)
    flat[pl.ds(FLAT_ROWS, SUB), :] = jnp.zeros((SUB, LANES), jnp.float32)
    row, left = offset // LANES, offset % LANES
    lane = lanes(OWN_BLOCK)
    turn = (LANES - left) % LANES

    def move(k):
        here = flat[pl.ds(row + k, OWN_BLOCK), :]
        after = flat[pl.ds(row + k + 1, OWN_BLOCK), :]
        out_ref[pl.ds(k, OWN_BLOCK), :] = pltpu.roll(jnp.where(lane >= left, here, after), turn, 1)

    blocks_of(OWN_ROWS, OWN_BLOCK, move)


def to_flat(tiles):
    square = pltpu.VMEM((LANES, LANES), jnp.float32)
    return pl.pallas_call(
        to_flat_kernel,
        name="to_flat",
        out_shape=jax.ShapeDtypeStruct((OWN_ROWS, LANES), jnp.float32),
        in_specs=[IN_VMEM],
        out_specs=IN_VMEM,
        scratch_shapes=[pltpu.VMEM((FLAT_ROWS + SUB, LANES), jnp.float32), square, square],
    )(tiles.reshape(FLAT_ROWS, LANES))


def to_tiles_kernel(before_ref, in_ref, out_ref, joined, flat, wide, tail):
    me, first = local_place()
    offset = me * SHARD - first * UNIT
    row, left = offset // LANES, offset % LANES
    lane = lanes(ROWS)

    def fill(ref, base, block):
        def move(k):
            joined[pl.ds(base + k, block), :] = pltpu.roll(ref[pl.ds(k, block), :], left, 1)
        return move

    blocks_of(HALO, ROWS, fill(before_ref, 0, ROWS))
    blocks_of(OWN_ROWS, OWN_BLOCK, fill(in_ref, HALO, OWN_BLOCK))
    joined[pl.ds(HALO + OWN_ROWS, FLAT_ROWS - OWN_ROWS), :] = jnp.zeros((FLAT_ROWS - OWN_ROWS, LANES), jnp.float32)

    def align(k):
        here = joined[pl.ds(HALO - row + k, ROWS), :]
        above = joined[pl.ds(HALO - 1 - row + k, ROWS), :]
        flat[pl.ds(k, ROWS), :] = jnp.where(lane >= left, here, above)

    blocks_of(FLAT_ROWS, ROWS, align)

    def pair(i, carry):
        unit = 2 * i
        u = first + unit

        @pl.when(among(u, Q))
        def _():
            narrow_to_tiles(flat, unit * ROWS, out_ref, unit, wide, 2 * EDGE)

        for j in range(2):
            unit_to_tiles(flat, (unit + j) * ROWS, out_ref, unit + j, u + j, wide, tail)
        return carry

    lax.fori_loop(0, COVER // 2, pair, 0)


def to_tiles(before, share):
    square = pltpu.VMEM((LANES, LANES), jnp.float32)
    return pl.pallas_call(
        to_tiles_kernel,
        name="to_tiles",
        out_shape=jax.ShapeDtypeStruct((COVER,) + TAIL, jnp.bfloat16),
        in_specs=[IN_VMEM, IN_VMEM],
        out_specs=IN_VMEM,
        scratch_shapes=[pltpu.VMEM((HALO + FLAT_ROWS, LANES), jnp.float32), pltpu.VMEM((FLAT_ROWS, LANES), jnp.float32), square, square],
    )(before, share)


def adam_step(grad_part, first_part, second_part, master_part, hyper_params, clip_scale, keep_decay):
    learn_rate, beta_one, beta_two, weight_decay = (hyper_params[k] for k in range(4))
    clipped = grad_part * clip_scale
    moment_one = beta_one * first_part + (1.0 - beta_one) * clipped
    moment_two = beta_two * second_part + (1.0 - beta_two) * (clipped * clipped)
    m_hat = moment_one / (1.0 - beta_one ** ADAM_STEP)
    v_hat = moment_two / (1.0 - beta_two ** ADAM_STEP)
    direction = m_hat / (jnp.sqrt(v_hat) + ADAM_EPS) + jnp.where(keep_decay, weight_decay * master_part, 0.0)
    new_master = master_part - learn_rate * direction
    return moment_one, moment_two, new_master


def row_tiles(mat):
    return mat.reshape(-1, SUB, TILES, LANES).transpose(0, 2, 1, 3)


def from_row_tiles(tiles):
    return tiles.transpose(0, 2, 1, 3).reshape(-1, WIDTH)


def solution(mesh):
    def local_update(*arrays):
        grads, (first_part, second_part, master_part, hyper_params) = arrays[:-4], arrays[-4:]
        me = lax.axis_index("dp")

        def tiles_of(tensor):
            arr, kind = grads[tensor], STARTS[tensor]
            if kind in (EMBED, OUT, DOWN):
                return row_tiles(arr.reshape(-1, WIDTH))
            width = arr.shape[-1]
            tiles = row_tiles(arr.reshape(LAYERS, WIDTH, width).transpose(0, 2, 1).reshape(-1, WIDTH))
            return tiles.reshape((LAYERS, width // SUB) + TAIL)

        tensors = [tiles_of(k) for k in range(TENSORS - 1)]
        blank = jnp.zeros(((END - NORMS) * UNIT - NORM_LEN,), jnp.bfloat16)
        small = jnp.concatenate([arr.reshape(-1) for arr in grads[TENSORS - 1:]] + [blank])
        tensors.append(small.reshape((END - NORMS,) + TAIL))
        grad_tiles, squares = reduce_scatter(pack(tensors))
        clip_scale = jnp.minimum(1.0, hyper_params[4] / (jnp.sqrt(squares[0]) + CLIP_EPS))
        grad_part = to_flat(grad_tiles).reshape(-1)[:SHARD]
        keep_decay = me * SHARD + lax.broadcasted_iota(jnp.int32, (SHARD,), 0) < SHARD * DEVICES - NORM_LEN
        moment_one, moment_two, new_master = adam_step(grad_part, first_part, second_part, master_part, hyper_params, clip_scale, keep_decay)
        before = lax.ppermute(new_master[SHARD - HALO * LANES:], "dp", [(r, r + 1) for r in range(DEVICES - 1)])
        padded = jnp.pad(new_master, (0, OWN_ROWS * LANES - SHARD))
        chunk = to_tiles(before.reshape(HALO, LANES), padded.reshape(OWN_ROWS, LANES))
        outs = unpack(all_gather(chunk), [t.shape for t in tensors])

        def tensor_of(tensor):
            tiles, dims = outs[tensor], grads[tensor].shape[1:]
            if STARTS[tensor] in (EMBED, OUT, DOWN):
                return from_row_tiles(tiles).reshape(dims)
            mat = from_row_tiles(tiles.reshape((-1,) + TAIL))
            return mat.reshape(LAYERS, dims[-1], WIDTH).transpose(0, 2, 1)

        results = [tensor_of(k) for k in range(TENSORS - 1)]
        flat_small, start = outs[-1].reshape(-1), 0
        for arr in grads[TENSORS - 1:]:
            size = math.prod(arr.shape)
            results.append(flat_small[start:start + size].reshape(arr.shape[1:]))
            start += size
        return tuple(results) + (moment_one, moment_two, new_master)

    in_specs = tuple([P("dp")] * 13 + [P()])
    out_specs = tuple([P()] * 10 + [P("dp"), P("dp"), P("dp")])
    return jax.shard_map(local_update, mesh=mesh, in_specs=in_specs, out_specs=out_specs, check_vma=False)
```

```python
import math
import jax
import jax.numpy as jnp
from jax import lax
from jax.sharding import PartitionSpec as P
from jax.experimental import pallas as pl
from jax.experimental.pallas import tpu as pltpu

ADAM_STEP = 7
ADAM_EPS = 1e-8
CLIP_EPS = 1e-6

SUB, LANES = 8, 128
TILES = 18
HALF = TILES // 2
ROWS = TILES * SUB
UNIT = ROWS * LANES
WIDTH = TILES * LANES
LAYERS = 6
DEVICES = 32
SHARD = 517920
NORM_LEN = 58368
TAIL = (TILES, SUB, LANES)
STARTS = (0, 500, 524, 536, 548, 572, 680, 788, 896, 900)
EMBED, Q, K, V, OUT, GATE, UP, DOWN, NORMS, END = STARTS
TENSORS = len(STARTS) - 1
COVER = 30
GATHER = 29
HALO = 2 * ROWS
OWN_ROWS = 4048
OWN_BLOCK = 176
FLAT_ROWS = COVER * ROWS
LINE = 4
SHIFTED = {17: 476, 18: 504}


def first_units():
    firsts = [SHIFTED.get(r, (r * SHARD) // UNIT) for r in range(DEVICES)]
    return firsts + [END]


FIRST = first_units()
COVER_FIRST = [min(first, END - COVER) for first in FIRST]
ANY = pl.BlockSpec(memory_space=pl.ANY)
IN_VMEM = pl.BlockSpec(memory_space=pltpu.VMEM)
IN_SMEM = pl.BlockSpec(memory_space=pltpu.SMEM)
BIG_VMEM = 66_000_000


def first_unit(r):
    value = r * (SHARD // math.gcd(SHARD, UNIT)) // (UNIT // math.gcd(SHARD, UNIT))
    for device, first in SHIFTED.items():
        value = jnp.where(r == device, first, value)
    return jnp.where(r == DEVICES, END, value)


def unit_runs(start, stop):
    runs = []
    for tensor in range(TENSORS):
        low, high = max(start, STARTS[tensor]), min(stop, STARTS[tensor + 1])
        if low < high:
            runs.append((tensor, low - STARTS[tensor], high - low, low - start))
    return runs


def tile_copies(refs, runs, slot_ref):
    pairs = []
    for tensor, first, count, slot in runs:
        ref = refs[tensor]
        kind = STARTS[tensor]
        if kind in (EMBED, OUT, DOWN, NORMS):
            pairs.append((ref.at[pl.ds(first, count)], slot_ref.at[pl.ds(slot, count)]))
        elif kind in (GATE, UP):
            for k in range(count):
                layer, col = divmod(first + k, TILES)
                pairs.append((ref.at[layer, :, col], slot_ref.at[slot + k]))
        else:
            per = 2 if kind == Q else 1
            for k in range(count):
                pair, odd = divmod(first + k, per)
                layer, half = divmod(pair, 2)
                for row in range(2):
                    part = slot_ref.at[slot + k, pl.ds(HALF * row, HALF)]
                    pairs.append((ref.at[layer, 2 * odd + row, pl.ds(HALF * half, HALF)], part))
    return pairs

SLOTS = 8


def unpack_kernel(*args):
    gathered, outs, (stage, in_sem, out_sem) = args[0], args[1:-3], args[-3:]
    depth = stage.shape[0]

    def wait_out(r):
        slot = r % depth
        count = FIRST[r + 1] - FIRST[r]
        part = stage.at[slot, pl.ds(0, count)]
        pltpu.make_async_copy(part, gathered.at[r, pl.ds(0, count)], out_sem.at[slot]).wait()

    def start_in(r):
        slot = r % depth
        if r >= depth:
            wait_out(r - depth)
        pltpu.make_async_copy(gathered.at[r], stage.at[slot], in_sem.at[slot]).start()

    ahead = depth // 2
    for r in range(ahead):
        start_in(r)
    for r in range(DEVICES):
        if r + ahead < DEVICES:
            start_in(r + ahead)
        slot = r % depth
        pltpu.make_async_copy(gathered.at[r], stage.at[slot], in_sem.at[slot]).wait()
        for dst, src in tile_copies(outs, unit_runs(FIRST[r], FIRST[r + 1]), stage.at[slot]):
            pltpu.make_async_copy(src, dst, out_sem.at[slot]).start()
    for r in range(DEVICES - depth, DEVICES):
        wait_out(r)


def unpack(gathered, tensor_shapes):
    return pl.pallas_call(
        unpack_kernel,
        name="unpack",
        out_shape=[jax.ShapeDtypeStruct(dims, jnp.bfloat16) for dims in tensor_shapes],
        in_specs=[ANY],
        out_specs=[ANY] * TENSORS,
        scratch_shapes=[
            pltpu.VMEM((SLOTS, GATHER) + TAIL, jnp.bfloat16),
            pltpu.SemaphoreType.DMA((SLOTS,)),
            pltpu.SemaphoreType.DMA((SLOTS,)),
        ],
        compiler_params=pltpu.CompilerParams(vmem_limit_bytes=BIG_VMEM),
    )(gathered)


def place():
    me = lax.axis_index("dp")
    return me // 8, (me // 4) % 2, (me // 2) % 2, me % 2


def index_of(z, y, x, c):
    return ((z * 2 + y) * 2 + x) * 2 + c


def greet(peers):
    barrier = pltpu.get_barrier_semaphore()
    for peer in peers:
        pl.semaphore_signal(barrier, inc=1, device_id=(peer,), device_id_type=pl.DeviceIdType.MESH)
    pl.semaphore_wait(barrier, len(peers))


def remote(src, dst, send, recv, peer):
    return pltpu.make_async_remote_copy(src_ref=src, dst_ref=dst, send_sem=send, recv_sem=recv, device_id=(peer,), device_id_type=pl.DeviceIdType.MESH)


class Sems:
    def __init__(self, send, recv):
        self.send, self.recv, self.used = send, recv, 0

    def copy(self, src, dst, peer):
        k = self.used
        self.used += 1
        return remote(src, dst, self.send.at[k], self.recv.at[k], peer)


COLORS = range(4)
OUTER = 8
DEPTH = 3


def jobs_of(plan):
    steps, first = [], 0
    for colors in plan:
        steps.append([(color, first + k, k) for k, color in enumerate(colors)])
        first += len(colors)
    return steps


RS_STEPS = jobs_of(((0, 1, 2), (0, 3, 2), (1, 2, 3), (0, 1, 3)) * 2 + ((0, 1, 2), (0, 1, 3)))


class Line:
    def __init__(self):
        z, y, x, c = place()
        self.inner = (z == 1) | (z == 2)
        self.end = jnp.logical_not(self.inner)
        self.near = z + 1 - 2 * (z % 2)
        self.cross = (z + 2) % LINE
        self.far = LINE - 1 - z
        self.peers = [index_of(zz, y, x, c) for zz in (self.near, self.cross, self.far)]


class Reduce:
    def __init__(self, job, slot, g_ref, stage, sum1, got1, got2, got3, send, recv):
        self.color, self.unit, k = job
        self.g_ref = g_ref
        z, y, x, c = place()
        self.z = z
        self.late = self.color >= 2
        by_x = self.color % 2 == 0
        self.mine = y if by_x else x
        if by_x:
            group = ((y, 1 - x, c), (y, 1 - x, 1 - c), (y, x, 1 - c))
            side = index_of(z, 1 - y, x, c)
            part = lambda yy, xx, cc: stage.at[slot, :, :, xx, cc, k]
        else:
            group = ((1 - y, x, c), (1 - y, x, 1 - c), (y, x, 1 - c))
            side = index_of(z, y, 1 - x, c)
            part = lambda yy, xx, cc: stage.at[slot, :, yy, :, cc, k]
        self.own = part(y, x, c)
        self.sum1 = sum1.at[k]
        self.got1, self.got2, self.got3 = got1, got2, got3
        sems = Sems(send, recv)
        self.copies1 = [sems.copy(part(*who), got1.at[i], index_of(z, *who)) for i, who in enumerate(group)]
        line = Line()
        self.line = line
        if self.late:
            self.side = sems.copy(got2.at[0, 1 - self.mine], got3.at[0], side)
            self.from_z, self.to_z = got2, lambda zz: self.sum1.at[zz]
        else:
            self.side = sems.copy(self.sum1.at[:, 1 - self.mine], got2, side)
            self.from_z, self.to_z = got3, lambda zz: got2.at[zz]
        near, cross, far = line.peers
        self.near = sems.copy(self.to_z(line.near), self.from_z.at[0], near)
        self.cross = sems.copy(self.to_z(line.cross), self.from_z.at[1], cross)
        self.direct = sems.copy(self.to_z(line.far), self.from_z.at[2], far)
        self.relay = sems.copy(self.to_z(line.far), self.from_z.at[3], near)

    def start_line(self):
        self.near.start()

        @pl.when(self.line.inner)
        def _():
            self.direct.start()

        @pl.when(self.line.end)
        def _():
            self.relay.start()
            self.cross.start()

    def pass_on(self):
        @pl.when(self.line.inner)
        def _():
            self.relay.wait_recv()
            held, more = self.to_z(self.line.cross), self.from_z.at[3]
            if self.late:
                for side in range(2):
                    held[side] = held[side] + more[side]
            else:
                held[...] = held[...] + more[...]
            self.cross.start()

    def recv_line(self):
        self.near.wait_recv()
        self.cross.wait_recv()

        @pl.when(self.line.inner)
        def _():
            self.direct.wait_recv()

    def line_total(self, pick):
        total = pick(self.to_z(self.z)) + pick(self.from_z.at[0]) + pick(self.from_z.at[1])
        return total + jnp.where(self.line.inner, pick(self.from_z.at[2]), 0.0)

    def sent_line(self):
        self.near.wait_send()
        self.cross.wait_send()

        @pl.when(self.line.inner)
        def _():
            self.direct.wait_send()

        @pl.when(self.line.end)
        def _():
            self.relay.wait_send()

    def sent_sums(self):
        if self.late:
            self.sent_line()
        else:
            self.side.wait_send()

    def sent_rest(self):
        if self.late:
            self.side.wait_send()
        else:
            self.sent_line()

    def phase0(self):
        recv_all(self.copies1)

        def body(i, carry):
            zz, side = i // 2, i % 2
            total = self.own[zz, side].astype(jnp.float32)
            for k in range(len(self.copies1)):
                total = total + self.got1[k, zz, side].astype(jnp.float32)
            self.sum1[zz, side] = total
            return carry

        lax.fori_loop(0, 2 * LINE, body, 0)
        return self.start_line if self.late else self.side.start

    def phase1(self):
        if self.late:
            self.pass_on()
            return None
        self.side.wait_recv()

        def body(zz, carry):
            self.got2[zz] = self.got2[zz] + self.sum1[zz, self.mine]
            return carry

        lax.fori_loop(0, LINE, body, 0)
        return self.start_line

    def phase2(self):
        if not self.late:
            self.pass_on()
            return None
        self.recv_line()
        for side in range(2):
            self.got2[0, side] = self.line_total(lambda ref: ref[side])
        return self.side.start

    def phase3(self, begin, end, acc):
        if self.late:
            self.side.wait_recv()
            total = self.got2[0, self.mine] + self.got3[0]
        else:
            self.recv_line()
            total = self.line_total(lambda ref: ref[...])
        mean = total * (1.0 / DEVICES)
        self.g_ref[self.unit] = mean
        square = jnp.sum(mean * mean, axis=0)
        return acc + jnp.where((self.unit >= begin) & (self.unit < end), square, 0.0)


def start_all(copies):
    for copy in copies:
        copy.start()


def recv_all(copies):
    for copy in copies:
        copy.wait_recv()


def send_all(copies):
    for copy in copies:
        copy.wait_send()


def reduce_kernel(*args):
    tensors, (g_ref, n_ref, stage, sum1, norm_buf, in_sem, send_n, recv_n) = args[:TENSORS], args[TENSORS:TENSORS + 8]
    rest = args[TENSORS + 8:]
    z, y, x, c = place()
    me = lax.axis_index("dp")
    steps = []
    for t, jobs in enumerate(RS_STEPS):
        steps.append([])
        for job in jobs:
            steps[t].append(Reduce(job, t % DEPTH, g_ref, stage, sum1.at[t % DEPTH], *rest[:5]))
            rest = rest[5:]
    count = len(steps)

    def start_in(t):
        if t < count:
            slot, first, units = t % DEPTH, steps[t][0].unit, len(steps[t])
            for r in range(DEVICES):
                zyx, core = divmod(r, 2)
                zy, xx = divmod(zyx, 2)
                zz, yy = divmod(zy, 2)
                runs = unit_runs(COVER_FIRST[r] + first, COVER_FIRST[r] + first + units)
                for src, dst in tile_copies(tensors, runs, stage.at[slot, zz, yy, xx, core]):
                    pltpu.make_async_copy(src, dst, in_sem.at[slot]).start()

    def start1(t):
        if t < count:
            part = stage.at[t % DEPTH, :, :, :, :, pl.ds(0, len(steps[t]))]
            pltpu.make_async_copy(part, part, in_sem.at[t % DEPTH]).wait()
            for k in range(3):
                for job in steps[t]:
                    job.copies1[k].start()

    for t in range(DEPTH):
        start_in(t)
    z_peers = Line().peers
    plane = [index_of(z, y, x, 1 - c), index_of(z, y, 1 - x, c), index_of(z, y, 1 - x, 1 - c), index_of(z, 1 - y, x, c), index_of(z, 1 - y, x, 1 - c)]
    greet(plane + z_peers)
    first = first_unit(me)
    begin = first - jnp.minimum(first, END - COVER)
    end = begin + first_unit(me + 1) - first
    acc = jnp.zeros((SUB, LANES), jnp.float32)
    start1(0)
    for t in range(count + 3):
        start1(t + 1)
        if t < count:
            if t >= DEPTH:
                for job in steps[t - DEPTH]:
                    job.sent_sums()
            start_all([Later(job.phase0()) for job in steps[t]])
            for job in steps[t]:
                send_all(job.copies1)
            start_in(t + DEPTH)
        if 1 <= t <= count:
            start_all([Later(job.phase1()) for job in steps[t - 1]])
        if 2 <= t <= count + 1:
            start_all([Later(job.phase2()) for job in steps[t - 2]])
        if t >= 3:
            for job in steps[t - 3]:
                acc = job.phase3(begin, end, acc)

    sems = Sems(send_n, recv_n)
    sent, used = [], 0
    norm_buf[0] = acc
    for peers in (z_peers, plane[:3], plane[3:4]):
        copies = [sems.copy(norm_buf.at[used], norm_buf.at[used + 1 + k], peer) for k, peer in enumerate(peers)]
        start_all(copies)
        recv_all(copies)
        sent += copies
        total = norm_buf[used]
        for k in range(len(peers)):
            total = total + norm_buf[used + 1 + k]
        used += 1 + len(peers)
        norm_buf[used] = total
    n_ref[0] = jnp.sum(norm_buf[used])

    send_all(sent)
    for t, jobs in enumerate(steps):
        for job in jobs:
            if t >= count - DEPTH:
                job.sent_sums()
            job.sent_rest()


class Later:
    def __init__(self, action):
        self.action = action

    def start(self):
        if self.action is not None:
            self.action()


def reduce_scatter(tensors):
    dma = pltpu.SemaphoreType.DMA
    scratch = []
    most = max(len(jobs) for jobs in RS_STEPS)
    for color, unit, k in sum(RS_STEPS, []):
        late = color >= 2
        scratch += [
            pltpu.VMEM((3, LINE, 2) + TAIL, jnp.bfloat16),
            pltpu.VMEM(((LINE, 2) if late else (LINE,)) + TAIL, jnp.float32),
            pltpu.VMEM((1 if late else LINE,) + TAIL, jnp.float32),
            dma((OUTER,)),
            dma((OUTER,)),
        ]
    return pl.pallas_call(
        reduce_kernel,
        name="reduce_scatter",
        out_shape=[jax.ShapeDtypeStruct((COVER,) + TAIL, jnp.float32), jax.ShapeDtypeStruct((1,), jnp.float32)],
        in_specs=[ANY] * TENSORS,
        out_specs=[IN_VMEM, IN_SMEM],
        scratch_shapes=[
            pltpu.VMEM((DEPTH, LINE, 2, 2, 2, most) + TAIL, jnp.bfloat16),
            pltpu.VMEM((DEPTH, most, LINE, 2) + TAIL, jnp.float32),
            pltpu.VMEM((11, SUB, LANES), jnp.float32),
            dma((DEPTH,)),
            dma((OUTER,)),
            dma((OUTER,)),
        ] + scratch,
        compiler_params=pltpu.CompilerParams(collective_id=0, has_side_effects=True, vmem_limit_bytes=BIG_VMEM),
    )(*tensors)


AG_STEPS = jobs_of(((0, 1, 2), (0, 1, 3)) * 4 + ((0, 1, 2), (0, 3)))


class Gather:
    def __init__(self, job, a_ref, b_ref, send, recv):
        color, unit, _ = job
        u = pl.ds(unit, 1)
        z, y, x, c = place()
        y_peer, x_peer, c_peer = index_of(z, 1 - y, x, c), index_of(z, y, 1 - x, c), index_of(z, y, x, 1 - c)
        by_x = color % 2 == 0
        side, last = (y_peer, x_peer) if by_x else (x_peer, y_peer)
        sems = Sems(send, recv)
        here, row = b_ref.at[z, y, x, c, u], b_ref.at[:, y, x, c, u]
        half = b_ref.at[:, :, x, c, u] if by_x else b_ref.at[:, y, :, c, u]
        full = b_ref.at[:, :, :, c, u]
        self.late = color >= 2
        if self.late:
            at = lambda zz: b_ref.at[zz, :, x, c, u] if by_x else b_ref.at[zz, y, :, c, u]
            source, self.side = at(z), sems.copy(a_ref.at[u], here, side)
        else:
            at = lambda zz: b_ref.at[zz, y, x, c, u]
            source, self.side = a_ref.at[u], sems.copy(row, row, side)
        self.line = line = Line()
        self.near, self.cross, self.direct = (sems.copy(source, at(z), peer) for peer in line.peers)
        self.relay = sems.copy(at(line.cross), at(line.cross), line.peers[0])
        self.half, self.full = sems.copy(half, half, last), sems.copy(full, full, c_peer)

    def start_line(self):
        self.near.start()
        self.cross.start()

        @pl.when(self.line.inner)
        def _():
            self.direct.start()

    def pass_on(self):
        @pl.when(self.line.inner)
        def _():
            self.cross.wait_recv()
            self.relay.start()

    def recv_line(self):
        self.near.wait_recv()

        @pl.when(self.line.inner)
        def _():
            self.direct.wait_recv()

        @pl.when(self.line.end)
        def _():
            self.cross.wait_recv()
            self.relay.wait_recv()

    def phases(self):
        nothing = lambda: None
        if self.late:
            first = [(nothing, self.side.start), (self.side.wait_recv, self.start_line), (nothing, self.pass_on), (self.recv_line, self.half.start)]
        else:
            first = [(nothing, self.start_line), (nothing, self.pass_on), (self.recv_line, self.side.start), (self.side.wait_recv, self.half.start)]
        return first + [(self.half.wait_recv, self.full.start), (self.full.wait_recv, nothing)]

    def sent(self):
        for copy in (self.side, self.near, self.cross, self.half, self.full):
            copy.wait_send()

        @pl.when(self.line.inner)
        def _():
            self.direct.wait_send()
            self.relay.wait_send()


def gather_kernel(a_ref, b_ref, own_sem, *rest):
    z, y, x, c = place()
    greet(Line().peers + [index_of(z, 1 - y, x, c), index_of(z, y, 1 - x, c), index_of(z, y, x, 1 - c)])
    own = pltpu.make_async_copy(a_ref.at[pl.ds(0, GATHER)], b_ref.at[z, y, x, c], own_sem)
    own.start()
    steps, made = [], []
    for jobs in AG_STEPS:
        steps.append([])
        for job in jobs:
            made.append(Gather(job, a_ref, b_ref, *rest[:2]))
            steps[-1].append(made[-1].phases())
            rest = rest[2:]
    count, phases = len(steps), len(steps[0][0])

    def run(t, phase):
        if 0 <= t < count:
            for job in steps[t]:
                job[phase][0]()
                job[phase][1]()

    run(0, 0)
    own.wait()
    for t in range(count + phases):
        run(t + 1, 0)
        for phase in range(1, phases):
            run(t + 1 - phase, phase)
    for job in made:
        job.sent()


def all_gather(chunk):
    dma = pltpu.SemaphoreType.DMA
    out = pl.pallas_call(
        gather_kernel,
        name="all_gather",
        out_shape=jax.ShapeDtypeStruct((LINE, 2, 2, 2, GATHER) + TAIL, jnp.bfloat16),
        in_specs=[IN_VMEM],
        out_specs=ANY,
        scratch_shapes=[dma] + [dma((OUTER,))] * (2 * len(sum(AG_STEPS, []))),
        compiler_params=pltpu.CompilerParams(collective_id=1, has_side_effects=True, vmem_limit_bytes=BIG_VMEM),
    )(chunk)
    return out.reshape((DEVICES, GATHER) + TAIL)


def lanes(rows):
    return lax.broadcasted_iota(jnp.int32, (rows, LANES), 1)


def among(u, *starts):
    found = False
    for start in starts:
        stop = STARTS[STARTS.index(start) + 1]
        found = ((u >= start) & (u < stop)) | found
    return found


def rolled(value, shift):
    shift = shift % LANES
    return value if shift == 0 else pltpu.roll(value, shift, 1)


def turned(tiles):
    blank = [jnp.zeros((SUB, LANES), jnp.float32)] * (LANES // SUB - len(tiles))
    return jnp.concatenate(tiles + blank, axis=0).T


def narrow_blocks(width):
    step = LANES // width
    return [(col, min(step, HALF - col)) for col in range(0, HALF, step)]


def tile(ref, unit, index):
    return ref.at[pl.ds(pl.multiple_of(unit * ROWS + index * SUB, SUB), SUB), :]


def narrow_to_flat(in_ref, unit, flat, row, wide, width):
    per, step, lane = width // SUB, LANES // width, lanes(width)
    for col, count in narrow_blocks(width):
        wide[...] = turned([tile(in_ref, unit, HALF * r + col + e)[...] for e in range(count) for r in range(per)])
        for e in range(count):
            value = None
            for j in range(step):
                pick = rolled(wide[pl.ds(j, width, stride=step), :], width * (j - e))
                value = pick if value is None else jnp.where(lane >= width * j, pick, value)
            flat[pl.ds(row + width * (col + e), width), :] = value


def narrow_to_tiles(flat, row, out_ref, unit, wide, width):
    per, step, lane = width // SUB, LANES // width, lanes(width)
    for col, count in narrow_blocks(width):
        for j in range(step):
            value = None
            for e in range(count):
                pick = rolled(flat[pl.ds(row + width * (col + e), width), :], width * (e - j))
                value = pick if value is None else jnp.where(lane >= width * e, pick, value)
            wide[pl.ds(j, width, stride=step), :] = value
        back = wide[...].T
        for e in range(count):
            for r in range(per):
                at = width * e + SUB * r
                index = HALF * r + col + e
                out_ref[unit + index // TILES, index % TILES] = back[at:at + SUB].astype(jnp.bfloat16)


EDGE = ROWS - LANES


def unit_to_flat(in_ref, unit, flat, row, u, wide, tail):
    @pl.when(among(u, EMBED, OUT, DOWN))
    def _():
        for e in range(SUB):
            flat[pl.ds(row + TILES * e, TILES), :] = in_ref[pl.ds(row + e, TILES, stride=SUB), :]

    @pl.when(among(u, NORMS))
    def _():
        flat[pl.ds(row, ROWS), :] = in_ref[pl.ds(row, ROWS), :]

    @pl.when(among(u, K, V))
    def _():
        narrow_to_flat(in_ref, unit, flat, row, wide, EDGE)

    @pl.when(among(u, GATE, UP))
    def _():
        wide[...] = turned([tile(in_ref, unit, t)[...] for t in range(LANES // SUB)])
        tail[...] = turned([tile(in_ref, unit, t)[...] for t in range(LANES // SUB, TILES)])
        lane = lanes(EDGE)
        before = None
        for j in range(SUB):
            head = rolled(wide[pl.ds(j, EDGE, stride=SUB), :], EDGE * j)
            rest = rolled(tail[pl.ds(j, EDGE, stride=SUB), :], EDGE * j)
            flat[pl.ds(row + j, EDGE, stride=HALF), :] = head if before is None else jnp.where(lane < EDGE * j, before, head)
            before = jnp.where((lane >= EDGE * j) & (lane < EDGE * (j + 1)), rest, head)
        flat[pl.ds(row + SUB, EDGE, stride=HALF), :] = before


def unit_to_tiles(flat, row, out_ref, unit, u, wide, tail):
    @pl.when(among(u, EMBED, OUT, DOWN))
    def _():
        for t in range(TILES):
            out_ref[unit, t] = flat[pl.ds(row + t, SUB, stride=TILES), :].astype(jnp.bfloat16)

    @pl.when(among(u, NORMS))
    def _():
        out_ref[unit] = flat[pl.ds(row, ROWS), :].reshape(TAIL).astype(jnp.bfloat16)

    @pl.when(among(u, K, V))
    def _():
        narrow_to_tiles(flat, row, out_ref, unit, wide, EDGE)

    @pl.when(among(u, GATE, UP))
    def _():
        lane = lanes(EDGE)
        for j in range(SUB):
            here = flat[pl.ds(row + j, EDGE, stride=HALF), :]
            after = flat[pl.ds(row + j + 1, EDGE, stride=HALF), :]
            wide[pl.ds(j, EDGE, stride=SUB), :] = rolled(jnp.where(lane >= EDGE * j, here, after), -EDGE * j)
            tail[pl.ds(j, EDGE, stride=SUB), :] = rolled(after, -EDGE * j)
        out_ref[unit, pl.ds(0, LANES // SUB)] = wide[...].T.reshape(LANES // SUB, SUB, LANES).astype(jnp.bfloat16)
        out_ref[unit, pl.ds(LANES // SUB, 2)] = tail[...].T[0:EDGE].reshape(2, SUB, LANES).astype(jnp.bfloat16)


def local_place():
    me = lax.axis_index("dp")
    return me, first_unit(me)


def blocks_of(rows, block, body):
    def step(i, carry):
        body(pl.multiple_of(i * block, SUB))
        return carry

    lax.fori_loop(0, rows // block, step, 0)


def to_flat_kernel(in_ref, out_ref, flat, wide, tail):
    me, first = local_place()
    first = jnp.minimum(first, END - COVER)
    offset = me * SHARD - first * UNIT

    def pair(i, carry):
        unit = 2 * i
        u = first + unit

        @pl.when(among(u, Q))
        def _():
            narrow_to_flat(in_ref, unit, flat, unit * ROWS, wide, 2 * EDGE)

        for j in range(2):
            unit_to_flat(in_ref, unit + j, flat, (unit + j) * ROWS, u + j, wide, tail)
        return carry

    lax.fori_loop(0, COVER // 2, pair, 0)
    flat[pl.ds(FLAT_ROWS, SUB), :] = jnp.zeros((SUB, LANES), jnp.float32)
    row, left = offset // LANES, offset % LANES
    lane = lanes(OWN_BLOCK)
    turn = (LANES - left) % LANES

    def move(k):
        here = flat[pl.ds(row + k, OWN_BLOCK), :]
        after = flat[pl.ds(row + k + 1, OWN_BLOCK), :]
        out_ref[pl.ds(k, OWN_BLOCK), :] = pltpu.roll(jnp.where(lane >= left, here, after), turn, 1)

    blocks_of(OWN_ROWS, OWN_BLOCK, move)


def to_flat(tiles):
    square = pltpu.VMEM((LANES, LANES), jnp.float32)
    return pl.pallas_call(
        to_flat_kernel,
        name="to_flat",
        out_shape=jax.ShapeDtypeStruct((OWN_ROWS, LANES), jnp.float32),
        in_specs=[IN_VMEM],
        out_specs=IN_VMEM,
        scratch_shapes=[pltpu.VMEM((FLAT_ROWS + SUB, LANES), jnp.float32), square, square],
    )(tiles.reshape(FLAT_ROWS, LANES))


def to_tiles_kernel(before_ref, in_ref, out_ref, joined, flat, wide, tail):
    me, first = local_place()
    offset = me * SHARD - first * UNIT
    row, left = offset // LANES, offset % LANES
    lane = lanes(ROWS)

    def fill(ref, base, block):
        def move(k):
            joined[pl.ds(base + k, block), :] = pltpu.roll(ref[pl.ds(k, block), :], left, 1)
        return move

    blocks_of(HALO, ROWS, fill(before_ref, 0, ROWS))
    blocks_of(OWN_ROWS, OWN_BLOCK, fill(in_ref, HALO, OWN_BLOCK))
    joined[pl.ds(HALO + OWN_ROWS, FLAT_ROWS - OWN_ROWS), :] = jnp.zeros((FLAT_ROWS - OWN_ROWS, LANES), jnp.float32)

    def align(k):
        here = joined[pl.ds(HALO - row + k, ROWS), :]
        above = joined[pl.ds(HALO - 1 - row + k, ROWS), :]
        flat[pl.ds(k, ROWS), :] = jnp.where(lane >= left, here, above)

    blocks_of(FLAT_ROWS, ROWS, align)

    def pair(i, carry):
        unit = 2 * i
        u = first + unit

        @pl.when(among(u, Q))
        def _():
            narrow_to_tiles(flat, unit * ROWS, out_ref, unit, wide, 2 * EDGE)

        for j in range(2):
            unit_to_tiles(flat, (unit + j) * ROWS, out_ref, unit + j, u + j, wide, tail)
        return carry

    lax.fori_loop(0, COVER // 2, pair, 0)


def to_tiles(before, share):
    square = pltpu.VMEM((LANES, LANES), jnp.float32)
    return pl.pallas_call(
        to_tiles_kernel,
        name="to_tiles",
        out_shape=jax.ShapeDtypeStruct((COVER,) + TAIL, jnp.bfloat16),
        in_specs=[IN_VMEM, IN_VMEM],
        out_specs=IN_VMEM,
        scratch_shapes=[pltpu.VMEM((HALO + FLAT_ROWS, LANES), jnp.float32), pltpu.VMEM((FLAT_ROWS, LANES), jnp.float32), square, square],
    )(before, share)


def adam_step(grad_part, first_part, second_part, master_part, hyper_params, clip_scale, keep_decay):
    learn_rate, beta_one, beta_two, weight_decay = (hyper_params[k] for k in range(4))
    clipped = grad_part * clip_scale
    moment_one = beta_one * first_part + (1.0 - beta_one) * clipped
    moment_two = beta_two * second_part + (1.0 - beta_two) * (clipped * clipped)
    m_hat = moment_one / (1.0 - beta_one ** ADAM_STEP)
    v_hat = moment_two / (1.0 - beta_two ** ADAM_STEP)
    direction = m_hat / (jnp.sqrt(v_hat) + ADAM_EPS) + jnp.where(keep_decay, weight_decay * master_part, 0.0)
    new_master = master_part - learn_rate * direction
    return moment_one, moment_two, new_master


def row_tiles(mat):
    return mat.reshape(-1, SUB, TILES, LANES).transpose(0, 2, 1, 3)


def from_row_tiles(tiles):
    return tiles.transpose(0, 2, 1, 3).reshape(-1, WIDTH)


def solution(mesh):
    def local_update(*arrays):
        grads, (first_part, second_part, master_part, hyper_params) = arrays[:-4], arrays[-4:]
        me = lax.axis_index("dp")

        def tiles_of(tensor):
            arr, kind = grads[tensor], STARTS[tensor]
            if kind in (EMBED, OUT, DOWN):
                return row_tiles(arr.reshape(-1, WIDTH))
            width = arr.shape[-1]
            tiles = row_tiles(arr.reshape(LAYERS, WIDTH, width).transpose(0, 2, 1).reshape(-1, WIDTH))
            return tiles.reshape((LAYERS, width // SUB) + TAIL)

        tensors = [tiles_of(k) for k in range(TENSORS - 1)]
        blank = jnp.zeros(((END - NORMS) * UNIT - NORM_LEN,), jnp.bfloat16)
        small = jnp.concatenate([arr.reshape(-1) for arr in grads[TENSORS - 1:]] + [blank])
        tensors.append(small.reshape((END - NORMS,) + TAIL))
        grad_tiles, squares = reduce_scatter(tensors)
        clip_scale = jnp.minimum(1.0, hyper_params[4] / (jnp.sqrt(squares[0]) + CLIP_EPS))
        grad_part = to_flat(grad_tiles).reshape(-1)[:SHARD]
        keep_decay = me * SHARD + lax.broadcasted_iota(jnp.int32, (SHARD,), 0) < SHARD * DEVICES - NORM_LEN
        moment_one, moment_two, new_master = adam_step(grad_part, first_part, second_part, master_part, hyper_params, clip_scale, keep_decay)
        before = lax.ppermute(new_master[SHARD - HALO * LANES:], "dp", [(r, r + 1) for r in range(DEVICES - 1)])
        padded = jnp.pad(new_master, (0, OWN_ROWS * LANES - SHARD))
        chunk = to_tiles(before.reshape(HALO, LANES), padded.reshape(OWN_ROWS, LANES))
        outs = unpack(all_gather(chunk), [t.shape for t in tensors])

        def tensor_of(tensor):
            tiles, dims = outs[tensor], grads[tensor].shape[1:]
            if STARTS[tensor] in (EMBED, OUT, DOWN):
                return from_row_tiles(tiles).reshape(dims)
            mat = from_row_tiles(tiles.reshape((-1,) + TAIL))
            return mat.reshape(LAYERS, dims[-1], WIDTH).transpose(0, 2, 1)

        results = [tensor_of(k) for k in range(TENSORS - 1)]
        flat_small, start = outs[-1].reshape(-1), 0
        for arr in grads[TENSORS - 1:]:
            size = math.prod(arr.shape)
            results.append(flat_small[start:start + size].reshape(arr.shape[1:]))
            start += size
        return tuple(results) + (moment_one, moment_two, new_master)

    in_specs = tuple([P("dp")] * 13 + [P()])
    out_specs = tuple([P()] * 10 + [P("dp"), P("dp"), P("dp")])
    return jax.shard_map(local_update, mesh=mesh, in_specs=in_specs, out_specs=out_specs, check_vma=False)
```

```python
import math
import jax
import jax.numpy as jnp
from jax import lax
from jax.sharding import PartitionSpec as P
from jax.experimental import pallas as pl
from jax.experimental.pallas import tpu as pltpu

ADAM_STEP = 7
ADAM_EPS = 1e-8
CLIP_EPS = 1e-6

SUB, LANES = 8, 128
TILES = 18
HALF = TILES // 2
ROWS = TILES * SUB
UNIT = ROWS * LANES
WIDTH = TILES * LANES
LAYERS = 6
DEVICES = 32
SHARD = 517920
NORM_LEN = 58368
TAIL = (TILES, SUB, LANES)
STARTS = (0, 500, 524, 536, 548, 572, 680, 788, 896, 900)
EMBED, Q, K, V, OUT, GATE, UP, DOWN, NORMS, END = STARTS
TENSORS = len(STARTS) - 1
COVER = 30
GATHER = 29
HALO = 2 * ROWS
OWN_ROWS = 4048
OWN_BLOCK = 176
FLAT_ROWS = COVER * ROWS
LINE = 4
SHIFTED = {17: 476, 18: 504}


def first_units():
    firsts = [SHIFTED.get(r, (r * SHARD) // UNIT) for r in range(DEVICES)]
    return firsts + [END]


FIRST = first_units()
COVER_FIRST = [min(first, END - COVER) for first in FIRST]
ANY = pl.BlockSpec(memory_space=pl.ANY)
IN_VMEM = pl.BlockSpec(memory_space=pltpu.VMEM)
IN_SMEM = pl.BlockSpec(memory_space=pltpu.SMEM)
BIG_VMEM = 66_000_000


def first_unit(r):
    value = r * (SHARD // math.gcd(SHARD, UNIT)) // (UNIT // math.gcd(SHARD, UNIT))
    for device, first in SHIFTED.items():
        value = jnp.where(r == device, first, value)
    return jnp.where(r == DEVICES, END, value)


def unit_runs(start, stop):
    runs = []
    for tensor in range(TENSORS):
        low, high = max(start, STARTS[tensor]), min(stop, STARTS[tensor + 1])
        if low < high:
            runs.append((tensor, low - STARTS[tensor], high - low, low - start))
    return runs


def tile_copies(refs, runs, slot_ref):
    pairs = []
    for tensor, first, count, slot in runs:
        ref = refs[tensor]
        kind = STARTS[tensor]
        if kind in (EMBED, OUT, DOWN, NORMS):
            pairs.append((ref.at[pl.ds(first, count)], slot_ref.at[pl.ds(slot, count)]))
        elif kind in (GATE, UP):
            for k in range(count):
                layer, col = divmod(first + k, TILES)
                pairs.append((ref.at[layer, :, col], slot_ref.at[slot + k]))
        else:
            per = 2 if kind == Q else 1
            for k in range(count):
                pair, odd = divmod(first + k, per)
                layer, half = divmod(pair, 2)
                for row in range(2):
                    part = slot_ref.at[slot + k, pl.ds(HALF * row, HALF)]
                    pairs.append((ref.at[layer, 2 * odd + row, pl.ds(HALF * half, HALF)], part))
    return pairs

SLOTS = 8


def unpack_kernel(*args):
    gathered, outs, (stage, in_sem, out_sem) = args[0], args[1:-3], args[-3:]
    depth = stage.shape[0]

    def wait_out(r):
        slot = r % depth
        count = FIRST[r + 1] - FIRST[r]
        part = stage.at[slot, pl.ds(0, count)]
        pltpu.make_async_copy(part, gathered.at[r, pl.ds(0, count)], out_sem.at[slot]).wait()

    def start_in(r):
        slot = r % depth
        if r >= depth:
            wait_out(r - depth)
        pltpu.make_async_copy(gathered.at[r], stage.at[slot], in_sem.at[slot]).start()

    ahead = depth // 2
    for r in range(ahead):
        start_in(r)
    for r in range(DEVICES):
        if r + ahead < DEVICES:
            start_in(r + ahead)
        slot = r % depth
        pltpu.make_async_copy(gathered.at[r], stage.at[slot], in_sem.at[slot]).wait()
        for dst, src in tile_copies(outs, unit_runs(FIRST[r], FIRST[r + 1]), stage.at[slot]):
            pltpu.make_async_copy(src, dst, out_sem.at[slot]).start()
    for r in range(DEVICES - depth, DEVICES):
        wait_out(r)


def unpack(gathered, tensor_shapes):
    return pl.pallas_call(
        unpack_kernel,
        name="unpack",
        out_shape=[jax.ShapeDtypeStruct(dims, jnp.bfloat16) for dims in tensor_shapes],
        in_specs=[ANY],
        out_specs=[ANY] * TENSORS,
        scratch_shapes=[
            pltpu.VMEM((SLOTS, GATHER) + TAIL, jnp.bfloat16),
            pltpu.SemaphoreType.DMA((SLOTS,)),
            pltpu.SemaphoreType.DMA((SLOTS,)),
        ],
        compiler_params=pltpu.CompilerParams(vmem_limit_bytes=BIG_VMEM),
    )(gathered)


def place():
    me = lax.axis_index("dp")
    return me // 8, (me // 4) % 2, (me // 2) % 2, me % 2


def index_of(z, y, x, c):
    return ((z * 2 + y) * 2 + x) * 2 + c


def greet(peers):
    barrier = pltpu.get_barrier_semaphore()
    for peer in peers:
        pl.semaphore_signal(barrier, inc=1, device_id=(peer,), device_id_type=pl.DeviceIdType.MESH)
    pl.semaphore_wait(barrier, len(peers))


def remote(src, dst, send, recv, peer):
    return pltpu.make_async_remote_copy(src_ref=src, dst_ref=dst, send_sem=send, recv_sem=recv, device_id=(peer,), device_id_type=pl.DeviceIdType.MESH)


class Sems:
    def __init__(self, send, recv):
        self.send, self.recv, self.used = send, recv, 0

    def copy(self, src, dst, peer):
        k = self.used
        self.used += 1
        return remote(src, dst, self.send.at[k], self.recv.at[k], peer)


COLORS = range(4)
OUTER = 8
DEPTH = 3
AHEAD = 1
PHASE = (0, 1, 3, 5)


def jobs_of(plan):
    steps, first = [], 0
    for colors in plan:
        steps.append([(color, first + k, k) for k, color in enumerate(colors)])
        first += len(colors)
    return steps


RS_STEPS = jobs_of(((0, 3), (2, 1), (2, 3)) * 5)


class Line:
    def __init__(self):
        z, y, x, c = place()
        self.inner = (z == 1) | (z == 2)
        self.end = jnp.logical_not(self.inner)
        self.near = z + 1 - 2 * (z % 2)
        self.cross = (z + 2) % LINE
        self.far = LINE - 1 - z
        self.peers = [index_of(zz, y, x, c) for zz in (self.near, self.cross, self.far)]


class Reduce:
    def __init__(self, job, slot, g_ref, stage, sum1, got1, got2, got3, send, recv):
        self.color, self.unit, k = job
        self.g_ref = g_ref
        z, y, x, c = place()
        self.z = z
        self.late = self.color >= 2
        by_x = self.color % 2 == 0
        self.mine = y if by_x else x
        if by_x:
            group = ((y, 1 - x, c), (y, 1 - x, 1 - c), (y, x, 1 - c))
            side = index_of(z, 1 - y, x, c)
            part = lambda yy, xx, cc: stage.at[slot, :, :, xx, cc, k]
        else:
            group = ((1 - y, x, c), (1 - y, x, 1 - c), (y, x, 1 - c))
            side = index_of(z, y, 1 - x, c)
            part = lambda yy, xx, cc: stage.at[slot, :, yy, :, cc, k]
        self.own = part(y, x, c)
        self.sum1 = sum1.at[k]
        self.got1, self.got2, self.got3 = got1, got2, got3
        sems = Sems(send, recv)
        self.copies1 = [sems.copy(part(*who), got1.at[i], index_of(z, *who)) for i, who in enumerate(group)]
        line = Line()
        self.line = line
        if self.late:
            self.side = sems.copy(got2.at[0, 1 - self.mine], got3.at[0], side)
            self.from_z, self.to_z = got2, lambda zz: self.sum1.at[zz]
        else:
            self.side = sems.copy(self.sum1.at[:, 1 - self.mine], got2, side)
            self.from_z, self.to_z = got3, lambda zz: got2.at[zz]
        near, cross, far = line.peers
        self.near = sems.copy(self.to_z(line.near), self.from_z.at[0], near)
        self.cross = sems.copy(self.to_z(line.cross), self.from_z.at[1], cross)
        self.direct = sems.copy(self.to_z(line.far), self.from_z.at[2], far)
        self.relay = sems.copy(self.to_z(line.far), self.from_z.at[3], near)

    def start_line(self):
        self.near.start()

        @pl.when(self.line.inner)
        def _():
            self.direct.start()

        @pl.when(self.line.end)
        def _():
            self.relay.start()
            self.cross.start()

    def pass_on(self):
        @pl.when(self.line.inner)
        def _():
            self.relay.wait_recv()
            held, more = self.to_z(self.line.cross), self.from_z.at[3]
            if self.late:
                for side in range(2):
                    held[side] = held[side] + more[side]
            else:
                held[...] = held[...] + more[...]
            self.cross.start()

    def recv_line(self):
        self.near.wait_recv()
        self.cross.wait_recv()

        @pl.when(self.line.inner)
        def _():
            self.direct.wait_recv()

    def line_total(self, pick):
        total = pick(self.to_z(self.z)) + pick(self.from_z.at[0]) + pick(self.from_z.at[1])
        return total + jnp.where(self.line.inner, pick(self.from_z.at[2]), 0.0)

    def sent_line(self):
        self.near.wait_send()
        self.cross.wait_send()

        @pl.when(self.line.inner)
        def _():
            self.direct.wait_send()

        @pl.when(self.line.end)
        def _():
            self.relay.wait_send()

    def sent_sums(self):
        if self.late:
            self.sent_line()
        else:
            self.side.wait_send()

    def sent_rest(self):
        if self.late:
            self.side.wait_send()
        else:
            self.sent_line()

    def phase0(self):
        recv_all(self.copies1)

        def body(i, carry):
            zz, side = i // 2, i % 2
            total = self.own[zz, side].astype(jnp.float32)
            for k in range(len(self.copies1)):
                total = total + self.got1[k, zz, side].astype(jnp.float32)
            self.sum1[zz, side] = total
            return carry

        lax.fori_loop(0, 2 * LINE, body, 0)
        return self.start_line if self.late else self.side.start

    def phase1(self):
        if self.late:
            self.pass_on()
            return None
        self.side.wait_recv()

        def body(zz, carry):
            self.got2[zz] = self.got2[zz] + self.sum1[zz, self.mine]
            return carry

        lax.fori_loop(0, LINE, body, 0)
        return self.start_line

    def phase2(self):
        if not self.late:
            self.pass_on()
            return None
        self.recv_line()
        for side in range(2):
            self.got2[0, side] = self.line_total(lambda ref: ref[side])
        return self.side.start

    def phase3(self, begin, end, acc):
        if self.late:
            self.side.wait_recv()
            total = self.got2[0, self.mine] + self.got3[0]
        else:
            self.recv_line()
            total = self.line_total(lambda ref: ref[...])
        mean = total * (1.0 / DEVICES)
        self.g_ref[self.unit] = mean
        square = jnp.sum(mean * mean, axis=0)
        return acc + jnp.where((self.unit >= begin) & (self.unit < end), square, 0.0)


def start_all(copies):
    for copy in copies:
        copy.start()


def recv_all(copies):
    for copy in copies:
        copy.wait_recv()


def send_all(copies):
    for copy in copies:
        copy.wait_send()


def reduce_kernel(*args):
    tensors, (g_ref, n_ref, stage, sum1, norm_buf, in_sem, send_n, recv_n) = args[:TENSORS], args[TENSORS:TENSORS + 8]
    rest = args[TENSORS + 8:]
    z, y, x, c = place()
    me = lax.axis_index("dp")
    steps, sums = [], PHASE[2] + 1
    for t, jobs in enumerate(RS_STEPS):
        steps.append([])
        for job in jobs:
            steps[t].append(Reduce(job, t % DEPTH, g_ref, stage, sum1.at[t % sums], *rest[:5]))
            rest = rest[5:]
    count = len(steps)

    def start_in(t):
        if t < count:
            slot, first, units = t % DEPTH, steps[t][0].unit, len(steps[t])
            for r in range(DEVICES):
                zyx, core = divmod(r, 2)
                zy, xx = divmod(zyx, 2)
                zz, yy = divmod(zy, 2)
                runs = unit_runs(COVER_FIRST[r] + first, COVER_FIRST[r] + first + units)
                for src, dst in tile_copies(tensors, runs, stage.at[slot, zz, yy, xx, core]):
                    pltpu.make_async_copy(src, dst, in_sem.at[slot]).start()

    def start1(t):
        if t < count:
            part = stage.at[t % DEPTH, :, :, :, :, pl.ds(0, len(steps[t]))]
            pltpu.make_async_copy(part, part, in_sem.at[t % DEPTH]).wait()
            for k in range(3):
                for job in steps[t]:
                    job.copies1[k].start()

    for t in range(DEPTH):
        start_in(t)
    z_peers = Line().peers
    plane = [index_of(z, y, x, 1 - c), index_of(z, y, 1 - x, c), index_of(z, y, 1 - x, 1 - c), index_of(z, 1 - y, x, c), index_of(z, 1 - y, x, 1 - c)]
    greet(plane + z_peers)
    first = first_unit(me)
    begin = first - jnp.minimum(first, END - COVER)
    end = begin + first_unit(me + 1) - first
    acc = jnp.zeros((SUB, LANES), jnp.float32)
    for t in range(AHEAD):
        start1(t)
    for t in range(count + PHASE[3]):
        start1(t + AHEAD)
        if t < count:
            if t >= sums:
                for job in steps[t - sums]:
                    job.sent_sums()
            start_all([Later(job.phase0()) for job in steps[t]])
            for job in steps[t]:
                send_all(job.copies1)
            start_in(t + DEPTH)
        if 0 <= t - PHASE[1] < count:
            start_all([Later(job.phase1()) for job in steps[t - PHASE[1]]])
        if 0 <= t - PHASE[2] < count:
            start_all([Later(job.phase2()) for job in steps[t - PHASE[2]]])
        if 0 <= t - PHASE[3]:
            for job in steps[t - PHASE[3]]:
                acc = job.phase3(begin, end, acc)

    sems = Sems(send_n, recv_n)
    sent, used = [], 0
    norm_buf[0] = acc
    for peers in (z_peers, plane[:3], plane[3:4]):
        copies = [sems.copy(norm_buf.at[used], norm_buf.at[used + 1 + k], peer) for k, peer in enumerate(peers)]
        start_all(copies)
        recv_all(copies)
        sent += copies
        total = norm_buf[used]
        for k in range(len(peers)):
            total = total + norm_buf[used + 1 + k]
        used += 1 + len(peers)
        norm_buf[used] = total
    n_ref[0] = jnp.sum(norm_buf[used])

    send_all(sent)
    for t, jobs in enumerate(steps):
        for job in jobs:
            if t >= count - sums:
                job.sent_sums()
            job.sent_rest()


class Later:
    def __init__(self, action):
        self.action = action

    def start(self):
        if self.action is not None:
            self.action()


def reduce_scatter(tensors):
    dma = pltpu.SemaphoreType.DMA
    scratch = []
    most = max(len(jobs) for jobs in RS_STEPS)
    for color, unit, k in sum(RS_STEPS, []):
        late = color >= 2
        scratch += [
            pltpu.VMEM((3, LINE, 2) + TAIL, jnp.bfloat16),
            pltpu.VMEM(((LINE, 2) if late else (LINE,)) + TAIL, jnp.float32),
            pltpu.VMEM((1 if late else LINE,) + TAIL, jnp.float32),
            dma((OUTER,)),
            dma((OUTER,)),
        ]
    return pl.pallas_call(
        reduce_kernel,
        name="reduce_scatter",
        out_shape=[jax.ShapeDtypeStruct((COVER,) + TAIL, jnp.float32), jax.ShapeDtypeStruct((1,), jnp.float32)],
        in_specs=[ANY] * TENSORS,
        out_specs=[IN_VMEM, IN_SMEM],
        scratch_shapes=[
            pltpu.VMEM((DEPTH, LINE, 2, 2, 2, most) + TAIL, jnp.bfloat16),
            pltpu.VMEM((PHASE[2] + 1, most, LINE, 2) + TAIL, jnp.float32),
            pltpu.VMEM((11, SUB, LANES), jnp.float32),
            dma((DEPTH,)),
            dma((OUTER,)),
            dma((OUTER,)),
        ] + scratch,
        compiler_params=pltpu.CompilerParams(collective_id=0, has_side_effects=True, vmem_limit_bytes=BIG_VMEM),
    )(*tensors)


AG_STEPS = jobs_of(((0, 3), (2, 1), (2, 3)) * 4 + ((0, 3), (2, 1), (2,)))


class Gather:
    def __init__(self, job, a_ref, b_ref, send, recv):
        color, unit, _ = job
        u = pl.ds(unit, 1)
        z, y, x, c = place()
        y_peer, x_peer, c_peer = index_of(z, 1 - y, x, c), index_of(z, y, 1 - x, c), index_of(z, y, x, 1 - c)
        by_x = color % 2 == 0
        side, last = (y_peer, x_peer) if by_x else (x_peer, y_peer)
        sems = Sems(send, recv)
        here, row = b_ref.at[z, y, x, c, u], b_ref.at[:, y, x, c, u]
        half = b_ref.at[:, :, x, c, u] if by_x else b_ref.at[:, y, :, c, u]
        full = b_ref.at[:, :, :, c, u]
        self.late = color >= 2
        if self.late:
            at = lambda zz: b_ref.at[zz, :, x, c, u] if by_x else b_ref.at[zz, y, :, c, u]
            source, self.side = at(z), sems.copy(a_ref.at[u], here, side)
        else:
            at = lambda zz: b_ref.at[zz, y, x, c, u]
            source, self.side = a_ref.at[u], sems.copy(row, row, side)
        self.line = line = Line()
        self.near, self.cross, self.direct = (sems.copy(source, at(z), peer) for peer in line.peers)
        self.relay = sems.copy(at(line.cross), at(line.cross), line.peers[0])
        self.half, self.full = sems.copy(half, half, last), sems.copy(full, full, c_peer)

    def start_line(self):
        self.near.start()
        self.cross.start()

        @pl.when(self.line.inner)
        def _():
            self.direct.start()

    def pass_on(self):
        @pl.when(self.line.inner)
        def _():
            self.cross.wait_recv()
            self.relay.start()

    def recv_line(self):
        self.near.wait_recv()

        @pl.when(self.line.inner)
        def _():
            self.direct.wait_recv()

        @pl.when(self.line.end)
        def _():
            self.cross.wait_recv()
            self.relay.wait_recv()

    def phases(self):
        nothing = lambda: None
        if self.late:
            first = [(nothing, self.side.start), (self.side.wait_recv, self.start_line), (nothing, self.pass_on), (self.recv_line, self.half.start)]
        else:
            first = [(nothing, self.start_line), (nothing, self.pass_on), (self.recv_line, self.side.start), (self.side.wait_recv, self.half.start)]
        return first + [(self.half.wait_recv, self.full.start), (self.full.wait_recv, nothing)]

    def sent(self):
        for copy in (self.side, self.near, self.cross, self.half, self.full):
            copy.wait_send()

        @pl.when(self.line.inner)
        def _():
            self.direct.wait_send()
            self.relay.wait_send()


def gather_kernel(a_ref, b_ref, own_sem, *rest):
    z, y, x, c = place()
    greet(Line().peers + [index_of(z, 1 - y, x, c), index_of(z, y, 1 - x, c), index_of(z, y, x, 1 - c)])
    own = pltpu.make_async_copy(a_ref.at[pl.ds(0, GATHER)], b_ref.at[z, y, x, c], own_sem)
    own.start()
    steps, made = [], []
    for jobs in AG_STEPS:
        steps.append([])
        for job in jobs:
            made.append(Gather(job, a_ref, b_ref, *rest[:2]))
            steps[-1].append(made[-1].phases())
            rest = rest[2:]
    count, phases = len(steps), len(steps[0][0])

    def run(t, phase):
        if 0 <= t < count:
            for job in steps[t]:
                job[phase][0]()
                job[phase][1]()

    run(0, 0)
    own.wait()
    for t in range(count + phases):
        run(t + 1, 0)
        for phase in range(1, phases):
            run(t + 1 - phase, phase)
    for job in made:
        job.sent()


def all_gather(chunk):
    dma = pltpu.SemaphoreType.DMA
    out = pl.pallas_call(
        gather_kernel,
        name="all_gather",
        out_shape=jax.ShapeDtypeStruct((LINE, 2, 2, 2, GATHER) + TAIL, jnp.bfloat16),
        in_specs=[IN_VMEM],
        out_specs=ANY,
        scratch_shapes=[dma] + [dma((OUTER,))] * (2 * len(sum(AG_STEPS, []))),
        compiler_params=pltpu.CompilerParams(collective_id=1, has_side_effects=True, vmem_limit_bytes=BIG_VMEM),
    )(chunk)
    return out.reshape((DEVICES, GATHER) + TAIL)


def lanes(rows):
    return lax.broadcasted_iota(jnp.int32, (rows, LANES), 1)


def among(u, *starts):
    found = False
    for start in starts:
        stop = STARTS[STARTS.index(start) + 1]
        found = ((u >= start) & (u < stop)) | found
    return found


def rolled(value, shift):
    shift = shift % LANES
    return value if shift == 0 else pltpu.roll(value, shift, 1)


def turned(tiles):
    blank = [jnp.zeros((SUB, LANES), jnp.float32)] * (LANES // SUB - len(tiles))
    return jnp.concatenate(tiles + blank, axis=0).T


def narrow_blocks(width):
    step = LANES // width
    return [(col, min(step, HALF - col)) for col in range(0, HALF, step)]


def tile(ref, unit, index):
    return ref.at[pl.ds(pl.multiple_of(unit * ROWS + index * SUB, SUB), SUB), :]


def narrow_to_flat(in_ref, unit, flat, row, wide, width):
    per, step, lane = width // SUB, LANES // width, lanes(width)
    for col, count in narrow_blocks(width):
        wide[...] = turned([tile(in_ref, unit, HALF * r + col + e)[...] for e in range(count) for r in range(per)])
        for e in range(count):
            value = None
            for j in range(step):
                pick = rolled(wide[pl.ds(j, width, stride=step), :], width * (j - e))
                value = pick if value is None else jnp.where(lane >= width * j, pick, value)
            flat[pl.ds(row + width * (col + e), width), :] = value


def narrow_to_tiles(flat, row, out_ref, unit, wide, width):
    per, step, lane = width // SUB, LANES // width, lanes(width)
    for col, count in narrow_blocks(width):
        for j in range(step):
            value = None
            for e in range(count):
                pick = rolled(flat[pl.ds(row + width * (col + e), width), :], width * (e - j))
                value = pick if value is None else jnp.where(lane >= width * e, pick, value)
            wide[pl.ds(j, width, stride=step), :] = value
        back = wide[...].T
        for e in range(count):
            for r in range(per):
                at = width * e + SUB * r
                index = HALF * r + col + e
                out_ref[unit + index // TILES, index % TILES] = back[at:at + SUB].astype(jnp.bfloat16)


EDGE = ROWS - LANES


def unit_to_flat(in_ref, unit, flat, row, u, wide, tail):
    @pl.when(among(u, EMBED, OUT, DOWN))
    def _():
        for e in range(SUB):
            flat[pl.ds(row + TILES * e, TILES), :] = in_ref[pl.ds(row + e, TILES, stride=SUB), :]

    @pl.when(among(u, NORMS))
    def _():
        flat[pl.ds(row, ROWS), :] = in_ref[pl.ds(row, ROWS), :]

    @pl.when(among(u, K, V))
    def _():
        narrow_to_flat(in_ref, unit, flat, row, wide, EDGE)

    @pl.when(among(u, GATE, UP))
    def _():
        wide[...] = turned([tile(in_ref, unit, t)[...] for t in range(LANES // SUB)])
        tail[...] = turned([tile(in_ref, unit, t)[...] for t in range(LANES // SUB, TILES)])
        lane = lanes(EDGE)
        before = None
        for j in range(SUB):
            head = rolled(wide[pl.ds(j, EDGE, stride=SUB), :], EDGE * j)
            rest = rolled(tail[pl.ds(j, EDGE, stride=SUB), :], EDGE * j)
            flat[pl.ds(row + j, EDGE, stride=HALF), :] = head if before is None else jnp.where(lane < EDGE * j, before, head)
            before = jnp.where((lane >= EDGE * j) & (lane < EDGE * (j + 1)), rest, head)
        flat[pl.ds(row + SUB, EDGE, stride=HALF), :] = before


def unit_to_tiles(flat, row, out_ref, unit, u, wide, tail):
    @pl.when(among(u, EMBED, OUT, DOWN))
    def _():
        for t in range(TILES):
            out_ref[unit, t] = flat[pl.ds(row + t, SUB, stride=TILES), :].astype(jnp.bfloat16)

    @pl.when(among(u, NORMS))
    def _():
        out_ref[unit] = flat[pl.ds(row, ROWS), :].reshape(TAIL).astype(jnp.bfloat16)

    @pl.when(among(u, K, V))
    def _():
        narrow_to_tiles(flat, row, out_ref, unit, wide, EDGE)

    @pl.when(among(u, GATE, UP))
    def _():
        lane = lanes(EDGE)
        for j in range(SUB):
            here = flat[pl.ds(row + j, EDGE, stride=HALF), :]
            after = flat[pl.ds(row + j + 1, EDGE, stride=HALF), :]
            wide[pl.ds(j, EDGE, stride=SUB), :] = rolled(jnp.where(lane >= EDGE * j, here, after), -EDGE * j)
            tail[pl.ds(j, EDGE, stride=SUB), :] = rolled(after, -EDGE * j)
        out_ref[unit, pl.ds(0, LANES // SUB)] = wide[...].T.reshape(LANES // SUB, SUB, LANES).astype(jnp.bfloat16)
        out_ref[unit, pl.ds(LANES // SUB, 2)] = tail[...].T[0:EDGE].reshape(2, SUB, LANES).astype(jnp.bfloat16)


def local_place():
    me = lax.axis_index("dp")
    return me, first_unit(me)


def blocks_of(rows, block, body):
    def step(i, carry):
        body(pl.multiple_of(i * block, SUB))
        return carry

    lax.fori_loop(0, rows // block, step, 0)


def to_flat_kernel(in_ref, out_ref, flat, wide, tail):
    me, first = local_place()
    first = jnp.minimum(first, END - COVER)
    offset = me * SHARD - first * UNIT

    def pair(i, carry):
        unit = 2 * i
        u = first + unit

        @pl.when(among(u, Q))
        def _():
            narrow_to_flat(in_ref, unit, flat, unit * ROWS, wide, 2 * EDGE)

        for j in range(2):
            unit_to_flat(in_ref, unit + j, flat, (unit + j) * ROWS, u + j, wide, tail)
        return carry

    lax.fori_loop(0, COVER // 2, pair, 0)
    flat[pl.ds(FLAT_ROWS, SUB), :] = jnp.zeros((SUB, LANES), jnp.float32)
    row, left = offset // LANES, offset % LANES
    lane = lanes(OWN_BLOCK)
    turn = (LANES - left) % LANES

    def move(k):
        here = flat[pl.ds(row + k, OWN_BLOCK), :]
        after = flat[pl.ds(row + k + 1, OWN_BLOCK), :]
        out_ref[pl.ds(k, OWN_BLOCK), :] = pltpu.roll(jnp.where(lane >= left, here, after), turn, 1)

    blocks_of(OWN_ROWS, OWN_BLOCK, move)


def to_flat(tiles):
    square = pltpu.VMEM((LANES, LANES), jnp.float32)
    return pl.pallas_call(
        to_flat_kernel,
        name="to_flat",
        out_shape=jax.ShapeDtypeStruct((OWN_ROWS, LANES), jnp.float32),
        in_specs=[IN_VMEM],
        out_specs=IN_VMEM,
        scratch_shapes=[pltpu.VMEM((FLAT_ROWS + SUB, LANES), jnp.float32), square, square],
    )(tiles.reshape(FLAT_ROWS, LANES))


def to_tiles_kernel(before_ref, in_ref, out_ref, joined, flat, wide, tail):
    me, first = local_place()
    offset = me * SHARD - first * UNIT
    row, left = offset // LANES, offset % LANES
    lane = lanes(ROWS)

    def fill(ref, base, block):
        def move(k):
            joined[pl.ds(base + k, block), :] = pltpu.roll(ref[pl.ds(k, block), :], left, 1)
        return move

    blocks_of(HALO, ROWS, fill(before_ref, 0, ROWS))
    blocks_of(OWN_ROWS, OWN_BLOCK, fill(in_ref, HALO, OWN_BLOCK))
    joined[pl.ds(HALO + OWN_ROWS, FLAT_ROWS - OWN_ROWS), :] = jnp.zeros((FLAT_ROWS - OWN_ROWS, LANES), jnp.float32)

    def align(k):
        here = joined[pl.ds(HALO - row + k, ROWS), :]
        above = joined[pl.ds(HALO - 1 - row + k, ROWS), :]
        flat[pl.ds(k, ROWS), :] = jnp.where(lane >= left, here, above)

    blocks_of(FLAT_ROWS, ROWS, align)

    def pair(i, carry):
        unit = 2 * i
        u = first + unit

        @pl.when(among(u, Q))
        def _():
            narrow_to_tiles(flat, unit * ROWS, out_ref, unit, wide, 2 * EDGE)

        for j in range(2):
            unit_to_tiles(flat, (unit + j) * ROWS, out_ref, unit + j, u + j, wide, tail)
        return carry

    lax.fori_loop(0, COVER // 2, pair, 0)


def to_tiles(before, share):
    square = pltpu.VMEM((LANES, LANES), jnp.float32)
    return pl.pallas_call(
        to_tiles_kernel,
        name="to_tiles",
        out_shape=jax.ShapeDtypeStruct((COVER,) + TAIL, jnp.bfloat16),
        in_specs=[IN_VMEM, IN_VMEM],
        out_specs=IN_VMEM,
        scratch_shapes=[pltpu.VMEM((HALO + FLAT_ROWS, LANES), jnp.float32), pltpu.VMEM((FLAT_ROWS, LANES), jnp.float32), square, square],
    )(before, share)


def adam_step(grad_part, first_part, second_part, master_part, hyper_params, clip_scale, keep_decay):
    learn_rate, beta_one, beta_two, weight_decay = (hyper_params[k] for k in range(4))
    clipped = grad_part * clip_scale
    moment_one = beta_one * first_part + (1.0 - beta_one) * clipped
    moment_two = beta_two * second_part + (1.0 - beta_two) * (clipped * clipped)
    m_hat = moment_one / (1.0 - beta_one ** ADAM_STEP)
    v_hat = moment_two / (1.0 - beta_two ** ADAM_STEP)
    direction = m_hat / (jnp.sqrt(v_hat) + ADAM_EPS) + jnp.where(keep_decay, weight_decay * master_part, 0.0)
    new_master = master_part - learn_rate * direction
    return moment_one, moment_two, new_master


def row_tiles(mat):
    return mat.reshape(-1, SUB, TILES, LANES).transpose(0, 2, 1, 3)


def from_row_tiles(tiles):
    return tiles.transpose(0, 2, 1, 3).reshape(-1, WIDTH)


def solution(mesh):
    def local_update(*arrays):
        grads, (first_part, second_part, master_part, hyper_params) = arrays[:-4], arrays[-4:]
        me = lax.axis_index("dp")

        def tiles_of(tensor):
            arr, kind = grads[tensor], STARTS[tensor]
            if kind in (EMBED, OUT, DOWN):
                return row_tiles(arr.reshape(-1, WIDTH))
            width = arr.shape[-1]
            tiles = row_tiles(arr.reshape(LAYERS, WIDTH, width).transpose(0, 2, 1).reshape(-1, WIDTH))
            return tiles.reshape((LAYERS, width // SUB) + TAIL)

        tensors = [tiles_of(k) for k in range(TENSORS - 1)]
        blank = jnp.zeros(((END - NORMS) * UNIT - NORM_LEN,), jnp.bfloat16)
        small = jnp.concatenate([arr.reshape(-1) for arr in grads[TENSORS - 1:]] + [blank])
        tensors.append(small.reshape((END - NORMS,) + TAIL))
        grad_tiles, squares = reduce_scatter(tensors)
        clip_scale = jnp.minimum(1.0, hyper_params[4] / (jnp.sqrt(squares[0]) + CLIP_EPS))
        grad_part = to_flat(grad_tiles).reshape(-1)[:SHARD]
        keep_decay = me * SHARD + lax.broadcasted_iota(jnp.int32, (SHARD,), 0) < SHARD * DEVICES - NORM_LEN
        moment_one, moment_two, new_master = adam_step(grad_part, first_part, second_part, master_part, hyper_params, clip_scale, keep_decay)
        before = lax.ppermute(new_master[SHARD - HALO * LANES:], "dp", [(r, r + 1) for r in range(DEVICES - 1)])
        padded = jnp.pad(new_master, (0, OWN_ROWS * LANES - SHARD))
        chunk = to_tiles(before.reshape(HALO, LANES), padded.reshape(OWN_ROWS, LANES))
        outs = unpack(all_gather(chunk), [t.shape for t in tensors])

        def tensor_of(tensor):
            tiles, dims = outs[tensor], grads[tensor].shape[1:]
            if STARTS[tensor] in (EMBED, OUT, DOWN):
                return from_row_tiles(tiles).reshape(dims)
            mat = from_row_tiles(tiles.reshape((-1,) + TAIL))
            return mat.reshape(LAYERS, dims[-1], WIDTH).transpose(0, 2, 1)

        results = [tensor_of(k) for k in range(TENSORS - 1)]
        flat_small, start = outs[-1].reshape(-1), 0
        for arr in grads[TENSORS - 1:]:
            size = math.prod(arr.shape)
            results.append(flat_small[start:start + size].reshape(arr.shape[1:]))
            start += size
        return tuple(results) + (moment_one, moment_two, new_master)

    in_specs = tuple([P("dp")] * 13 + [P()])
    out_specs = tuple([P()] * 10 + [P("dp"), P("dp"), P("dp")])
    return jax.shard_map(local_update, mesh=mesh, in_specs=in_specs, out_specs=out_specs, check_vma=False)
```

```python
import math
import jax
import jax.numpy as jnp
from jax import lax
from jax.sharding import PartitionSpec as P
from jax.experimental import pallas as pl
from jax.experimental.pallas import tpu as pltpu

ADAM_STEP = 7
ADAM_EPS = 1e-8
CLIP_EPS = 1e-6

SUB, LANES = 8, 128
TILES = 18
HALF = TILES // 2
ROWS = TILES * SUB
UNIT = ROWS * LANES
WIDTH = TILES * LANES
LAYERS = 6
DEVICES = 32
SHARD = 517920
NORM_LEN = 58368
TAIL = (TILES, SUB, LANES)
STARTS = (0, 500, 524, 536, 548, 572, 680, 788, 896, 900)
EMBED, Q, K, V, OUT, GATE, UP, DOWN, NORMS, END = STARTS
TENSORS = len(STARTS) - 1
COVER = 30
GATHER = 29
HALO = 2 * ROWS
OWN_ROWS = 4048
OWN_BLOCK = 176
FLAT_ROWS = COVER * ROWS
LINE = 4
SHIFTED = {17: 476, 18: 504}


def first_units():
    firsts = [SHIFTED.get(r, (r * SHARD) // UNIT) for r in range(DEVICES)]
    return firsts + [END]


FIRST = first_units()
COVER_FIRST = [min(first, END - COVER) for first in FIRST]
ANY = pl.BlockSpec(memory_space=pl.ANY)
IN_VMEM = pl.BlockSpec(memory_space=pltpu.VMEM)
IN_SMEM = pl.BlockSpec(memory_space=pltpu.SMEM)
BIG_VMEM = 66_000_000


def first_unit(r):
    value = r * (SHARD // math.gcd(SHARD, UNIT)) // (UNIT // math.gcd(SHARD, UNIT))
    for device, first in SHIFTED.items():
        value = jnp.where(r == device, first, value)
    return jnp.where(r == DEVICES, END, value)


def unit_runs(start, stop):
    runs = []
    for tensor in range(TENSORS):
        low, high = max(start, STARTS[tensor]), min(stop, STARTS[tensor + 1])
        if low < high:
            runs.append((tensor, low - STARTS[tensor], high - low, low - start))
    return runs


def tile_copies(refs, runs, slot_ref):
    pairs = []
    for tensor, first, count, slot in runs:
        ref = refs[tensor]
        kind = STARTS[tensor]
        if kind in (EMBED, OUT, DOWN, NORMS):
            pairs.append((ref.at[pl.ds(first, count)], slot_ref.at[pl.ds(slot, count)]))
        elif kind in (GATE, UP):
            for k in range(count):
                layer, col = divmod(first + k, TILES)
                pairs.append((ref.at[layer, :, col], slot_ref.at[slot + k]))
        else:
            per = 2 if kind == Q else 1
            for k in range(count):
                pair, odd = divmod(first + k, per)
                layer, half = divmod(pair, 2)
                for row in range(2):
                    part = slot_ref.at[slot + k, pl.ds(HALF * row, HALF)]
                    pairs.append((ref.at[layer, 2 * odd + row, pl.ds(HALF * half, HALF)], part))
    return pairs

SLOTS = 8


def unpack_kernel(*args):
    gathered, outs, (stage, in_sem, out_sem) = args[0], args[1:-3], args[-3:]
    depth = stage.shape[0]

    def wait_out(r):
        slot = r % depth
        count = FIRST[r + 1] - FIRST[r]
        part = stage.at[slot, pl.ds(0, count)]
        pltpu.make_async_copy(part, gathered.at[r, pl.ds(0, count)], out_sem.at[slot]).wait()

    def start_in(r):
        slot = r % depth
        if r >= depth:
            wait_out(r - depth)
        pltpu.make_async_copy(gathered.at[r], stage.at[slot], in_sem.at[slot]).start()

    ahead = depth // 2
    for r in range(ahead):
        start_in(r)
    for r in range(DEVICES):
        if r + ahead < DEVICES:
            start_in(r + ahead)
        slot = r % depth
        pltpu.make_async_copy(gathered.at[r], stage.at[slot], in_sem.at[slot]).wait()
        for dst, src in tile_copies(outs, unit_runs(FIRST[r], FIRST[r + 1]), stage.at[slot]):
            pltpu.make_async_copy(src, dst, out_sem.at[slot]).start()
    for r in range(DEVICES - depth, DEVICES):
        wait_out(r)


def unpack(gathered, tensor_shapes):
    return pl.pallas_call(
        unpack_kernel,
        name="unpack",
        out_shape=[jax.ShapeDtypeStruct(dims, jnp.bfloat16) for dims in tensor_shapes],
        in_specs=[ANY],
        out_specs=[ANY] * TENSORS,
        scratch_shapes=[
            pltpu.VMEM((SLOTS, GATHER) + TAIL, jnp.bfloat16),
            pltpu.SemaphoreType.DMA((SLOTS,)),
            pltpu.SemaphoreType.DMA((SLOTS,)),
        ],
        compiler_params=pltpu.CompilerParams(vmem_limit_bytes=BIG_VMEM),
    )(gathered)


def place():
    me = lax.axis_index("dp")
    return me // 8, (me // 4) % 2, (me // 2) % 2, me % 2


def index_of(z, y, x, c):
    return ((z * 2 + y) * 2 + x) * 2 + c


def greet(peers):
    barrier = pltpu.get_barrier_semaphore()
    for peer in peers:
        pl.semaphore_signal(barrier, inc=1, device_id=(peer,), device_id_type=pl.DeviceIdType.MESH)
    pl.semaphore_wait(barrier, len(peers))


def remote(src, dst, send, recv, peer):
    return pltpu.make_async_remote_copy(src_ref=src, dst_ref=dst, send_sem=send, recv_sem=recv, device_id=(peer,), device_id_type=pl.DeviceIdType.MESH)


class Sems:
    def __init__(self, send, recv):
        self.send, self.recv, self.used = send, recv, 0

    def copy(self, src, dst, peer):
        k = self.used
        self.used += 1
        return remote(src, dst, self.send.at[k], self.recv.at[k], peer)


COLORS = range(4)
OUTER = 8
DEPTH = 3
AHEAD = 1
PHASE = (0, 1, 3, 5)


def jobs_of(plan):
    steps, first = [], 0
    for colors in plan:
        steps.append([(color, first + k, k) for k, color in enumerate(colors)])
        first += len(colors)
    return steps


RS_STEPS = jobs_of(((2, 3), (0, 3), (2, 1)) * 5)


class Line:
    def __init__(self):
        z, y, x, c = place()
        self.inner = (z == 1) | (z == 2)
        self.end = jnp.logical_not(self.inner)
        self.near = z + 1 - 2 * (z % 2)
        self.cross = (z + 2) % LINE
        self.far = LINE - 1 - z
        self.peers = [index_of(zz, y, x, c) for zz in (self.near, self.cross, self.far)]


class Reduce:
    def __init__(self, job, slot, g_ref, stage, sum1, got1, got2, got3, send, recv):
        self.color, self.unit, k = job
        self.g_ref = g_ref
        z, y, x, c = place()
        self.z = z
        self.late = self.color >= 2
        by_x = self.color % 2 == 0
        self.mine = y if by_x else x
        if by_x:
            group = ((y, 1 - x, c), (y, 1 - x, 1 - c), (y, x, 1 - c))
            side = index_of(z, 1 - y, x, c)
            part = lambda yy, xx, cc: stage.at[slot, :, :, xx, cc, k]
        else:
            group = ((1 - y, x, c), (1 - y, x, 1 - c), (y, x, 1 - c))
            side = index_of(z, y, 1 - x, c)
            part = lambda yy, xx, cc: stage.at[slot, :, yy, :, cc, k]
        self.own = part(y, x, c)
        self.sum1 = sum1.at[k]
        self.got1, self.got2, self.got3 = got1, got2, got3
        sems = Sems(send, recv)
        self.copies1 = [sems.copy(part(*who), got1.at[i], index_of(z, *who)) for i, who in enumerate(group)]
        line = Line()
        self.line = line
        if self.late:
            self.side = sems.copy(got2.at[0, 1 - self.mine], got3.at[0], side)
            self.from_z, self.to_z = got2, lambda zz: self.sum1.at[zz]
        else:
            self.side = sems.copy(self.sum1.at[:, 1 - self.mine], got2, side)
            self.from_z, self.to_z = got3, lambda zz: got2.at[zz]
        near, cross, far = line.peers
        self.near = sems.copy(self.to_z(line.near), self.from_z.at[0], near)
        self.cross = sems.copy(self.to_z(line.cross), self.from_z.at[1], cross)
        self.direct = sems.copy(self.to_z(line.far), self.from_z.at[2], far)
        self.relay = sems.copy(self.to_z(line.far), self.from_z.at[3], near)

    def start_line(self):
        self.near.start()

        @pl.when(self.line.inner)
        def _():
            self.direct.start()

        @pl.when(self.line.end)
        def _():
            self.relay.start()
            self.cross.start()

    def pass_on(self):
        @pl.when(self.line.inner)
        def _():
            self.relay.wait_recv()
            held, more = self.to_z(self.line.cross), self.from_z.at[3]
            if self.late:
                for side in range(2):
                    held[side] = held[side] + more[side]
            else:
                held[...] = held[...] + more[...]
            self.cross.start()

    def recv_line(self):
        self.near.wait_recv()
        self.cross.wait_recv()

        @pl.when(self.line.inner)
        def _():
            self.direct.wait_recv()

    def line_total(self, pick):
        total = pick(self.to_z(self.z)) + pick(self.from_z.at[0]) + pick(self.from_z.at[1])
        return total + jnp.where(self.line.inner, pick(self.from_z.at[2]), 0.0)

    def sent_line(self):
        self.near.wait_send()
        self.cross.wait_send()

        @pl.when(self.line.inner)
        def _():
            self.direct.wait_send()

        @pl.when(self.line.end)
        def _():
            self.relay.wait_send()

    def sent_sums(self):
        if self.late:
            self.sent_line()
        else:
            self.side.wait_send()

    def sent_rest(self):
        if self.late:
            self.side.wait_send()
        else:
            self.sent_line()

    def phase0(self):
        recv_all(self.copies1)

        def body(i, carry):
            zz, side = i // 2, i % 2
            total = self.own[zz, side].astype(jnp.float32)
            for k in range(len(self.copies1)):
                total = total + self.got1[k, zz, side].astype(jnp.float32)
            self.sum1[zz, side] = total
            return carry

        lax.fori_loop(0, 2 * LINE, body, 0)
        return self.start_line if self.late else self.side.start

    def phase1(self):
        if self.late:
            self.pass_on()
            return None
        self.side.wait_recv()

        def body(zz, carry):
            self.got2[zz] = self.got2[zz] + self.sum1[zz, self.mine]
            return carry

        lax.fori_loop(0, LINE, body, 0)
        return self.start_line

    def phase2(self):
        if not self.late:
            self.pass_on()
            return None
        self.recv_line()
        for side in range(2):
            self.got2[0, side] = self.line_total(lambda ref: ref[side])
        return self.side.start

    def phase3(self, begin, end, acc):
        if self.late:
            self.side.wait_recv()
            total = self.got2[0, self.mine] + self.got3[0]
        else:
            self.recv_line()
            total = self.line_total(lambda ref: ref[...])
        mean = total * (1.0 / DEVICES)
        self.g_ref[self.unit] = mean
        square = jnp.sum(mean * mean, axis=0)
        return acc + jnp.where((self.unit >= begin) & (self.unit < end), square, 0.0)


def start_all(copies):
    for copy in copies:
        copy.start()


def recv_all(copies):
    for copy in copies:
        copy.wait_recv()


def send_all(copies):
    for copy in copies:
        copy.wait_send()


def reduce_kernel(*args):
    tensors, (g_ref, n_ref, stage, sum1, norm_buf, in_sem, send_n, recv_n) = args[:TENSORS], args[TENSORS:TENSORS + 8]
    rest = args[TENSORS + 8:]
    z, y, x, c = place()
    me = lax.axis_index("dp")
    steps, sums = [], PHASE[2] + 1
    for t, jobs in enumerate(RS_STEPS):
        steps.append([])
        for job in jobs:
            steps[t].append(Reduce(job, t % DEPTH, g_ref, stage, sum1.at[t % sums], *rest[:5]))
            rest = rest[5:]
    count = len(steps)

    def start_in(t):
        if t < count:
            slot, first, units = t % DEPTH, steps[t][0].unit, len(steps[t])
            for r in range(DEVICES):
                zyx, core = divmod(r, 2)
                zy, xx = divmod(zyx, 2)
                zz, yy = divmod(zy, 2)
                runs = unit_runs(COVER_FIRST[r] + first, COVER_FIRST[r] + first + units)
                for src, dst in tile_copies(tensors, runs, stage.at[slot, zz, yy, xx, core]):
                    pltpu.make_async_copy(src, dst, in_sem.at[slot]).start()

    def start1(t):
        if t < count:
            part = stage.at[t % DEPTH, :, :, :, :, pl.ds(0, len(steps[t]))]
            pltpu.make_async_copy(part, part, in_sem.at[t % DEPTH]).wait()
            for k in range(3):
                for job in steps[t]:
                    job.copies1[k].start()

    for t in range(DEPTH):
        start_in(t)
    z_peers = Line().peers
    plane = [index_of(z, y, x, 1 - c), index_of(z, y, 1 - x, c), index_of(z, y, 1 - x, 1 - c), index_of(z, 1 - y, x, c), index_of(z, 1 - y, x, 1 - c)]
    greet(plane + z_peers)
    first = first_unit(me)
    begin = first - jnp.minimum(first, END - COVER)
    end = begin + first_unit(me + 1) - first
    acc = jnp.zeros((SUB, LANES), jnp.float32)
    for t in range(AHEAD):
        start1(t)
    for t in range(count + PHASE[3]):
        start1(t + AHEAD)
        if t < count:
            if t >= sums:
                for job in steps[t - sums]:
                    job.sent_sums()
            start_all([Later(job.phase0()) for job in steps[t]])
            for job in steps[t]:
                send_all(job.copies1)
            start_in(t + DEPTH)
        if 0 <= t - PHASE[1] < count:
            start_all([Later(job.phase1()) for job in steps[t - PHASE[1]]])
        if 0 <= t - PHASE[2] < count:
            start_all([Later(job.phase2()) for job in steps[t - PHASE[2]]])
        if 0 <= t - PHASE[3]:
            for job in steps[t - PHASE[3]]:
                acc = job.phase3(begin, end, acc)

    sems = Sems(send_n, recv_n)
    sent, used = [], 0
    norm_buf[0] = acc
    for peers in (z_peers, plane[:3], plane[3:4]):
        copies = [sems.copy(norm_buf.at[used], norm_buf.at[used + 1 + k], peer) for k, peer in enumerate(peers)]
        start_all(copies)
        recv_all(copies)
        sent += copies
        total = norm_buf[used]
        for k in range(len(peers)):
            total = total + norm_buf[used + 1 + k]
        used += 1 + len(peers)
        norm_buf[used] = total
    n_ref[0] = jnp.sum(norm_buf[used])

    send_all(sent)
    for t, jobs in enumerate(steps):
        for job in jobs:
            if t >= count - sums:
                job.sent_sums()
            job.sent_rest()


class Later:
    def __init__(self, action):
        self.action = action

    def start(self):
        if self.action is not None:
            self.action()


def reduce_scatter(tensors):
    dma = pltpu.SemaphoreType.DMA
    scratch = []
    most = max(len(jobs) for jobs in RS_STEPS)
    for color, unit, k in sum(RS_STEPS, []):
        late = color >= 2
        scratch += [
            pltpu.VMEM((3, LINE, 2) + TAIL, jnp.bfloat16),
            pltpu.VMEM(((LINE, 2) if late else (LINE,)) + TAIL, jnp.float32),
            pltpu.VMEM((1 if late else LINE,) + TAIL, jnp.float32),
            dma((OUTER,)),
            dma((OUTER,)),
        ]
    return pl.pallas_call(
        reduce_kernel,
        name="reduce_scatter",
        out_shape=[jax.ShapeDtypeStruct((COVER,) + TAIL, jnp.float32), jax.ShapeDtypeStruct((1,), jnp.float32)],
        in_specs=[ANY] * TENSORS,
        out_specs=[IN_VMEM, IN_SMEM],
        scratch_shapes=[
            pltpu.VMEM((DEPTH, LINE, 2, 2, 2, most) + TAIL, jnp.bfloat16),
            pltpu.VMEM((PHASE[2] + 1, most, LINE, 2) + TAIL, jnp.float32),
            pltpu.VMEM((11, SUB, LANES), jnp.float32),
            dma((DEPTH,)),
            dma((OUTER,)),
            dma((OUTER,)),
        ] + scratch,
        compiler_params=pltpu.CompilerParams(collective_id=0, has_side_effects=True, vmem_limit_bytes=BIG_VMEM),
    )(*tensors)


AG_STEPS = jobs_of(((0, 3), (2, 1), (2, 3)) * 4 + ((0, 3), (2, 1), (2,)))


class Gather:
    def __init__(self, job, a_ref, b_ref, send, recv):
        color, unit, _ = job
        u = pl.ds(unit, 1)
        z, y, x, c = place()
        y_peer, x_peer, c_peer = index_of(z, 1 - y, x, c), index_of(z, y, 1 - x, c), index_of(z, y, x, 1 - c)
        by_x = color % 2 == 0
        side, last = (y_peer, x_peer) if by_x else (x_peer, y_peer)
        sems = Sems(send, recv)
        here, row = b_ref.at[z, y, x, c, u], b_ref.at[:, y, x, c, u]
        half = b_ref.at[:, :, x, c, u] if by_x else b_ref.at[:, y, :, c, u]
        full = b_ref.at[:, :, :, c, u]
        self.late = color >= 2
        if self.late:
            at = lambda zz: b_ref.at[zz, :, x, c, u] if by_x else b_ref.at[zz, y, :, c, u]
            source, self.side = at(z), sems.copy(a_ref.at[u], here, side)
        else:
            at = lambda zz: b_ref.at[zz, y, x, c, u]
            source, self.side = a_ref.at[u], sems.copy(row, row, side)
        self.line = line = Line()
        self.near, self.cross, self.direct = (sems.copy(source, at(z), peer) for peer in line.peers)
        self.relay = sems.copy(at(line.cross), at(line.cross), line.peers[0])
        self.half, self.full = sems.copy(half, half, last), sems.copy(full, full, c_peer)

    def start_line(self):
        self.near.start()
        self.cross.start()

        @pl.when(self.line.inner)
        def _():
            self.direct.start()

    def pass_on(self):
        @pl.when(self.line.inner)
        def _():
            self.cross.wait_recv()
            self.relay.start()

    def recv_line(self):
        self.near.wait_recv()

        @pl.when(self.line.inner)
        def _():
            self.direct.wait_recv()

        @pl.when(self.line.end)
        def _():
            self.cross.wait_recv()
            self.relay.wait_recv()

    def phases(self):
        nothing = lambda: None
        if self.late:
            first = [(nothing, self.side.start), (self.side.wait_recv, self.start_line), (nothing, self.pass_on), (self.recv_line, self.half.start)]
        else:
            first = [(nothing, self.start_line), (nothing, self.pass_on), (self.recv_line, self.side.start), (self.side.wait_recv, self.half.start)]
        return first + [(self.half.wait_recv, self.full.start), (self.full.wait_recv, nothing)]

    def sent(self):
        for copy in (self.side, self.near, self.cross, self.half, self.full):
            copy.wait_send()

        @pl.when(self.line.inner)
        def _():
            self.direct.wait_send()
            self.relay.wait_send()


def gather_kernel(a_ref, b_ref, own_sem, *rest):
    z, y, x, c = place()
    greet(Line().peers + [index_of(z, 1 - y, x, c), index_of(z, y, 1 - x, c), index_of(z, y, x, 1 - c)])
    own = pltpu.make_async_copy(a_ref.at[pl.ds(0, GATHER)], b_ref.at[z, y, x, c], own_sem)
    own.start()
    steps, made = [], []
    for jobs in AG_STEPS:
        steps.append([])
        for job in jobs:
            made.append(Gather(job, a_ref, b_ref, *rest[:2]))
            steps[-1].append(made[-1].phases())
            rest = rest[2:]
    count, phases = len(steps), len(steps[0][0])

    def run(t, phase):
        if 0 <= t < count:
            for job in steps[t]:
                job[phase][0]()
                job[phase][1]()

    run(0, 0)
    own.wait()
    for t in range(count + phases):
        run(t + 1, 0)
        for phase in range(1, phases):
            run(t + 1 - phase, phase)
    for job in made:
        job.sent()


def all_gather(chunk):
    dma = pltpu.SemaphoreType.DMA
    out = pl.pallas_call(
        gather_kernel,
        name="all_gather",
        out_shape=jax.ShapeDtypeStruct((LINE, 2, 2, 2, GATHER) + TAIL, jnp.bfloat16),
        in_specs=[IN_VMEM],
        out_specs=ANY,
        scratch_shapes=[dma] + [dma((OUTER,))] * (2 * len(sum(AG_STEPS, []))),
        compiler_params=pltpu.CompilerParams(collective_id=1, has_side_effects=True, vmem_limit_bytes=BIG_VMEM),
    )(chunk)
    return out.reshape((DEVICES, GATHER) + TAIL)


def lanes(rows):
    return lax.broadcasted_iota(jnp.int32, (rows, LANES), 1)


def among(u, *starts):
    found = False
    for start in starts:
        stop = STARTS[STARTS.index(start) + 1]
        found = ((u >= start) & (u < stop)) | found
    return found


def rolled(value, shift):
    shift = shift % LANES
    return value if shift == 0 else pltpu.roll(value, shift, 1)


def turned(tiles):
    blank = [jnp.zeros((SUB, LANES), jnp.float32)] * (LANES // SUB - len(tiles))
    return jnp.concatenate(tiles + blank, axis=0).T


def narrow_blocks(width):
    step = LANES // width
    return [(col, min(step, HALF - col)) for col in range(0, HALF, step)]


def tile(ref, unit, index):
    return ref.at[pl.ds(pl.multiple_of(unit * ROWS + index * SUB, SUB), SUB), :]


def narrow_to_flat(in_ref, unit, flat, row, wide, width):
    per, step, lane = width // SUB, LANES // width, lanes(width)
    for col, count in narrow_blocks(width):
        wide[...] = turned([tile(in_ref, unit, HALF * r + col + e)[...] for e in range(count) for r in range(per)])
        for e in range(count):
            value = None
            for j in range(step):
                pick = rolled(wide[pl.ds(j, width, stride=step), :], width * (j - e))
                value = pick if value is None else jnp.where(lane >= width * j, pick, value)
            flat[pl.ds(row + width * (col + e), width), :] = value


def narrow_to_tiles(flat, row, out_ref, unit, wide, width):
    per, step, lane = width // SUB, LANES // width, lanes(width)
    for col, count in narrow_blocks(width):
        for j in range(step):
            value = None
            for e in range(count):
                pick = rolled(flat[pl.ds(row + width * (col + e), width), :], width * (e - j))
                value = pick if value is None else jnp.where(lane >= width * e, pick, value)
            wide[pl.ds(j, width, stride=step), :] = value
        back = wide[...].T
        for e in range(count):
            for r in range(per):
                at = width * e + SUB * r
                index = HALF * r + col + e
                out_ref[unit + index // TILES, index % TILES] = back[at:at + SUB].astype(jnp.bfloat16)


EDGE = ROWS - LANES


def unit_to_flat(in_ref, unit, flat, row, u, wide, tail):
    @pl.when(among(u, EMBED, OUT, DOWN))
    def _():
        for e in range(SUB):
            flat[pl.ds(row + TILES * e, TILES), :] = in_ref[pl.ds(row + e, TILES, stride=SUB), :]

    @pl.when(among(u, NORMS))
    def _():
        flat[pl.ds(row, ROWS), :] = in_ref[pl.ds(row, ROWS), :]

    @pl.when(among(u, K, V))
    def _():
        narrow_to_flat(in_ref, unit, flat, row, wide, EDGE)

    @pl.when(among(u, GATE, UP))
    def _():
        wide[...] = turned([tile(in_ref, unit, t)[...] for t in range(LANES // SUB)])
        tail[:, 0:EDGE] = jnp.concatenate([tile(in_ref, unit, t)[...] for t in range(LANES // SUB, TILES)], axis=0).T
        lane = lanes(EDGE)
        before = None
        for j in range(SUB):
            head = rolled(wide[pl.ds(j, EDGE, stride=SUB), :], EDGE * j)
            rest = rolled(tail[pl.ds(j, EDGE, stride=SUB), :], EDGE * j)
            flat[pl.ds(row + j, EDGE, stride=HALF), :] = head if before is None else jnp.where(lane < EDGE * j, before, head)
            before = jnp.where((lane >= EDGE * j) & (lane < EDGE * (j + 1)), rest, head)
        flat[pl.ds(row + SUB, EDGE, stride=HALF), :] = before


def unit_to_tiles(flat, row, out_ref, unit, u, wide, tail):
    @pl.when(among(u, EMBED, OUT, DOWN))
    def _():
        for t in range(TILES):
            out_ref[unit, t] = flat[pl.ds(row + t, SUB, stride=TILES), :].astype(jnp.bfloat16)

    @pl.when(among(u, NORMS))
    def _():
        out_ref[unit] = flat[pl.ds(row, ROWS), :].reshape(TAIL).astype(jnp.bfloat16)

    @pl.when(among(u, K, V))
    def _():
        narrow_to_tiles(flat, row, out_ref, unit, wide, EDGE)

    @pl.when(among(u, GATE, UP))
    def _():
        lane = lanes(EDGE)
        for j in range(SUB):
            here = flat[pl.ds(row + j, EDGE, stride=HALF), :]
            after = flat[pl.ds(row + j + 1, EDGE, stride=HALF), :]
            wide[pl.ds(j, EDGE, stride=SUB), :] = rolled(jnp.where(lane >= EDGE * j, here, after), -EDGE * j)
            tail[pl.ds(j, EDGE, stride=SUB), :] = rolled(after, -EDGE * j)
        out_ref[unit, pl.ds(0, LANES // SUB)] = wide[...].T.reshape(LANES // SUB, SUB, LANES).astype(jnp.bfloat16)
        out_ref[unit, pl.ds(LANES // SUB, 2)] = tail[:, 0:EDGE].T.reshape(2, SUB, LANES).astype(jnp.bfloat16)


def local_place():
    me = lax.axis_index("dp")
    return me, first_unit(me)


def blocks_of(rows, block, body):
    def step(i, carry):
        body(pl.multiple_of(i * block, SUB))
        return carry

    lax.fori_loop(0, rows // block, step, 0)


def to_flat_kernel(in_ref, out_ref, flat, wide, tail):
    me, first = local_place()
    first = jnp.minimum(first, END - COVER)
    offset = me * SHARD - first * UNIT

    def pair(i, carry):
        unit = 2 * i
        u = first + unit

        @pl.when(among(u, Q))
        def _():
            narrow_to_flat(in_ref, unit, flat, unit * ROWS, wide, 2 * EDGE)

        for j in range(2):
            unit_to_flat(in_ref, unit + j, flat, (unit + j) * ROWS, u + j, wide, tail)
        return carry

    lax.fori_loop(0, COVER // 2, pair, 0)
    flat[pl.ds(FLAT_ROWS, SUB), :] = jnp.zeros((SUB, LANES), jnp.float32)
    row, left = offset // LANES, offset % LANES
    lane = lanes(OWN_BLOCK)
    turn = (LANES - left) % LANES

    def move(k):
        here = flat[pl.ds(row + k, OWN_BLOCK), :]
        after = flat[pl.ds(row + k + 1, OWN_BLOCK), :]
        out_ref[pl.ds(k, OWN_BLOCK), :] = pltpu.roll(jnp.where(lane >= left, here, after), turn, 1)

    blocks_of(OWN_ROWS, OWN_BLOCK, move)


def to_flat(tiles):
    square = pltpu.VMEM((LANES, LANES), jnp.float32)
    return pl.pallas_call(
        to_flat_kernel,
        name="to_flat",
        out_shape=jax.ShapeDtypeStruct((OWN_ROWS, LANES), jnp.float32),
        in_specs=[IN_VMEM],
        out_specs=IN_VMEM,
        scratch_shapes=[pltpu.VMEM((FLAT_ROWS + SUB, LANES), jnp.float32), square, square],
    )(tiles.reshape(FLAT_ROWS, LANES))


def to_tiles_kernel(before_ref, in_ref, out_ref, joined, flat, wide, tail):
    me, first = local_place()
    offset = me * SHARD - first * UNIT
    row, left = offset // LANES, offset % LANES
    lane = lanes(ROWS)

    def fill(ref, base, block):
        def move(k):
            joined[pl.ds(base + k, block), :] = pltpu.roll(ref[pl.ds(k, block), :], left, 1)
        return move

    blocks_of(HALO, ROWS, fill(before_ref, 0, ROWS))
    blocks_of(OWN_ROWS, OWN_BLOCK, fill(in_ref, HALO, OWN_BLOCK))
    joined[pl.ds(HALO + OWN_ROWS, FLAT_ROWS - OWN_ROWS), :] = jnp.zeros((FLAT_ROWS - OWN_ROWS, LANES), jnp.float32)

    def align(k):
        here = joined[pl.ds(HALO - row + k, ROWS), :]
        above = joined[pl.ds(HALO - 1 - row + k, ROWS), :]
        flat[pl.ds(k, ROWS), :] = jnp.where(lane >= left, here, above)

    blocks_of(FLAT_ROWS, ROWS, align)

    def pair(i, carry):
        unit = 2 * i
        u = first + unit

        @pl.when(among(u, Q))
        def _():
            narrow_to_tiles(flat, unit * ROWS, out_ref, unit, wide, 2 * EDGE)

        for j in range(2):
            unit_to_tiles(flat, (unit + j) * ROWS, out_ref, unit + j, u + j, wide, tail)
        return carry

    lax.fori_loop(0, COVER // 2, pair, 0)


def to_tiles(before, share):
    square = pltpu.VMEM((LANES, LANES), jnp.float32)
    return pl.pallas_call(
        to_tiles_kernel,
        name="to_tiles",
        out_shape=jax.ShapeDtypeStruct((COVER,) + TAIL, jnp.bfloat16),
        in_specs=[IN_VMEM, IN_VMEM],
        out_specs=IN_VMEM,
        scratch_shapes=[pltpu.VMEM((HALO + FLAT_ROWS, LANES), jnp.float32), pltpu.VMEM((FLAT_ROWS, LANES), jnp.float32), square, square],
    )(before, share)


def adam_step(grad_part, first_part, second_part, master_part, hyper_params, clip_scale, keep_decay):
    learn_rate, beta_one, beta_two, weight_decay = (hyper_params[k] for k in range(4))
    rest, warm = 1.0 - hyper_params, 1.0 - hyper_params ** ADAM_STEP
    rest_one, rest_two, warm_one, warm_two = rest[1], rest[2], warm[1], warm[2]
    clipped = grad_part * clip_scale
    moment_one = beta_one * first_part + rest_one * clipped
    moment_two = beta_two * second_part + rest_two * (clipped * clipped)
    m_hat = moment_one / warm_one
    v_hat = moment_two / warm_two
    direction = m_hat / (jnp.sqrt(v_hat) + ADAM_EPS) + jnp.where(keep_decay, weight_decay * master_part, 0.0)
    new_master = master_part - learn_rate * direction
    return moment_one, moment_two, new_master


def row_tiles(mat):
    return mat.reshape(-1, SUB, TILES, LANES).transpose(0, 2, 1, 3)


def from_row_tiles(tiles):
    return tiles.transpose(0, 2, 1, 3).reshape(-1, WIDTH)


def solution(mesh):
    def local_update(*arrays):
        grads, (first_part, second_part, master_part, hyper_params) = arrays[:-4], arrays[-4:]
        me = lax.axis_index("dp")

        def tiles_of(tensor):
            arr, kind = grads[tensor], STARTS[tensor]
            if kind in (EMBED, OUT, DOWN):
                return row_tiles(arr.reshape(-1, WIDTH))
            width = arr.shape[-1]
            tiles = row_tiles(arr.reshape(LAYERS, WIDTH, width).transpose(0, 2, 1).reshape(-1, WIDTH))
            return tiles.reshape((LAYERS, width // SUB) + TAIL)

        tensors = [tiles_of(k) for k in range(TENSORS - 1)]
        blank = jnp.zeros(((END - NORMS) * UNIT - NORM_LEN,), jnp.bfloat16)
        small = jnp.concatenate([arr.reshape(-1) for arr in grads[TENSORS - 1:]] + [blank])
        tensors.append(small.reshape((END - NORMS,) + TAIL))
        grad_tiles, squares = reduce_scatter(tensors)
        clip_scale = jnp.minimum(1.0, hyper_params[4] / (jnp.sqrt(squares[0]) + CLIP_EPS))
        grad_part = to_flat(grad_tiles).reshape(-1)[:SHARD]
        keep_decay = me * SHARD + lax.broadcasted_iota(jnp.int32, (SHARD,), 0) < SHARD * DEVICES - NORM_LEN
        moment_one, moment_two, new_master = adam_step(grad_part, first_part, second_part, master_part, hyper_params, clip_scale, keep_decay)
        before = lax.ppermute(new_master[SHARD - HALO * LANES:], "dp", [(r, r + 1) for r in range(DEVICES - 1)])
        padded = jnp.pad(new_master, (0, OWN_ROWS * LANES - SHARD))
        chunk = to_tiles(before.reshape(HALO, LANES), padded.reshape(OWN_ROWS, LANES))
        outs = unpack(all_gather(chunk), [t.shape for t in tensors])

        def tensor_of(tensor):
            tiles, dims = outs[tensor], grads[tensor].shape[1:]
            if STARTS[tensor] in (EMBED, OUT, DOWN):
                return from_row_tiles(tiles).reshape(dims)
            mat = from_row_tiles(tiles.reshape((-1,) + TAIL))
            return mat.reshape(LAYERS, dims[-1], WIDTH).transpose(0, 2, 1)

        results = [tensor_of(k) for k in range(TENSORS - 1)]
        flat_small, start = outs[-1].reshape(-1), 0
        for arr in grads[TENSORS - 1:]:
            size = math.prod(arr.shape)
            results.append(flat_small[start:start + size].reshape(arr.shape[1:]))
            start += size
        return tuple(results) + (moment_one, moment_two, new_master)

    in_specs = tuple([P("dp")] * 13 + [P()])
    out_specs = tuple([P()] * 10 + [P("dp"), P("dp"), P("dp")])
    return jax.shard_map(local_update, mesh=mesh, in_specs=in_specs, out_specs=out_specs, check_vma=False)
```

```python
import math
import jax
import jax.numpy as jnp
from jax import lax
from jax.sharding import PartitionSpec as P
from jax.experimental import pallas as pl
from jax.experimental.pallas import tpu as pltpu

ADAM_STEP = 7
ADAM_EPS = 1e-8
CLIP_EPS = 1e-6

SUB, LANES = 8, 128
TILES = 18
HALF = TILES // 2
ROWS = TILES * SUB
UNIT = ROWS * LANES
WIDTH = TILES * LANES
LAYERS = 6
DEVICES = 32
SHARD = 517920
NORM_LEN = 58368
TAIL = (TILES, SUB, LANES)
STARTS = (0, 500, 524, 536, 548, 572, 680, 788, 896, 900)
EMBED, Q, K, V, OUT, GATE, UP, DOWN, NORMS, END = STARTS
TENSORS = len(STARTS) - 1
COVER = 30
GATHER = 29
HALO = 2 * ROWS
OWN_ROWS = 4048
OWN_BLOCK = 176
FLAT_ROWS = COVER * ROWS
LINE = 4
SHIFTED = {17: 476, 18: 504}


def first_units():
    firsts = [SHIFTED.get(r, (r * SHARD) // UNIT) for r in range(DEVICES)]
    return firsts + [END]


FIRST = first_units()
COVER_FIRST = [min(first, END - COVER) for first in FIRST]
ANY = pl.BlockSpec(memory_space=pl.ANY)
IN_VMEM = pl.BlockSpec(memory_space=pltpu.VMEM)
IN_SMEM = pl.BlockSpec(memory_space=pltpu.SMEM)
BIG_VMEM = 66_000_000


def first_unit(r):
    value = r * (SHARD // math.gcd(SHARD, UNIT)) // (UNIT // math.gcd(SHARD, UNIT))
    for device, first in SHIFTED.items():
        value = jnp.where(r == device, first, value)
    return jnp.where(r == DEVICES, END, value)


def unit_runs(start, stop):
    runs = []
    for tensor in range(TENSORS):
        low, high = max(start, STARTS[tensor]), min(stop, STARTS[tensor + 1])
        if low < high:
            runs.append((tensor, low - STARTS[tensor], high - low, low - start))
    return runs


def tile_copies(refs, runs, slot_ref):
    pairs = []
    for tensor, first, count, slot in runs:
        ref = refs[tensor]
        kind = STARTS[tensor]
        if kind in (EMBED, OUT, DOWN, NORMS):
            pairs.append((ref.at[pl.ds(first, count)], slot_ref.at[pl.ds(slot, count)]))
        elif kind in (GATE, UP):
            for k in range(count):
                layer, col = divmod(first + k, TILES)
                pairs.append((ref.at[layer, :, col], slot_ref.at[slot + k]))
        else:
            per = 2 if kind == Q else 1
            for k in range(count):
                pair, odd = divmod(first + k, per)
                layer, half = divmod(pair, 2)
                for row in range(2):
                    part = slot_ref.at[slot + k, pl.ds(HALF * row, HALF)]
                    pairs.append((ref.at[layer, 2 * odd + row, pl.ds(HALF * half, HALF)], part))
    return pairs

SLOTS = 8


def unpack_kernel(*args):
    gathered, outs, (stage, in_sem, out_sem) = args[0], args[1:-3], args[-3:]
    depth = stage.shape[0]

    def wait_out(r):
        slot = r % depth
        count = FIRST[r + 1] - FIRST[r]
        part = stage.at[slot, pl.ds(0, count)]
        pltpu.make_async_copy(part, gathered.at[r, pl.ds(0, count)], out_sem.at[slot]).wait()

    def start_in(r):
        slot = r % depth
        if r >= depth:
            wait_out(r - depth)
        pltpu.make_async_copy(gathered.at[r], stage.at[slot], in_sem.at[slot]).start()

    ahead = depth // 2
    for r in range(ahead):
        start_in(r)
    for r in range(DEVICES):
        if r + ahead < DEVICES:
            start_in(r + ahead)
        slot = r % depth
        pltpu.make_async_copy(gathered.at[r], stage.at[slot], in_sem.at[slot]).wait()
        for dst, src in tile_copies(outs, unit_runs(FIRST[r], FIRST[r + 1]), stage.at[slot]):
            pltpu.make_async_copy(src, dst, out_sem.at[slot]).start()
    for r in range(DEVICES - depth, DEVICES):
        wait_out(r)


def unpack(gathered, tensor_shapes):
    return pl.pallas_call(
        unpack_kernel,
        name="unpack",
        out_shape=[jax.ShapeDtypeStruct(dims, jnp.bfloat16) for dims in tensor_shapes],
        in_specs=[ANY],
        out_specs=[ANY] * TENSORS,
        scratch_shapes=[
            pltpu.VMEM((SLOTS, GATHER) + TAIL, jnp.bfloat16),
            pltpu.SemaphoreType.DMA((SLOTS,)),
            pltpu.SemaphoreType.DMA((SLOTS,)),
        ],
        compiler_params=pltpu.CompilerParams(vmem_limit_bytes=BIG_VMEM),
    )(gathered)


def place():
    me = lax.axis_index("dp")
    return me // 8, (me // 4) % 2, (me // 2) % 2, me % 2


def index_of(z, y, x, c):
    return ((z * 2 + y) * 2 + x) * 2 + c


def greet(peers):
    barrier = pltpu.get_barrier_semaphore()
    for peer in peers:
        pl.semaphore_signal(barrier, inc=1, device_id=(peer,), device_id_type=pl.DeviceIdType.MESH)
    pl.semaphore_wait(barrier, len(peers))


def remote(src, dst, send, recv, peer):
    return pltpu.make_async_remote_copy(src_ref=src, dst_ref=dst, send_sem=send, recv_sem=recv, device_id=(peer,), device_id_type=pl.DeviceIdType.MESH)


class Sems:
    def __init__(self, send, recv):
        self.send, self.recv, self.used = send, recv, 0

    def copy(self, src, dst, peer):
        k = self.used
        self.used += 1
        return remote(src, dst, self.send.at[k], self.recv.at[k], peer)


COLORS = range(4)
OUTER = 8
NORM_SLOTS = 13
DEPTH = 3
AHEAD = 1
PHASE = (0, 1, 3, 5)


def jobs_of(plan):
    steps, first = [], 0
    for colors in plan:
        steps.append([(color, first + k, k) for k, color in enumerate(colors)])
        first += len(colors)
    return steps


RS_STEPS = jobs_of(((2, 3), (0, 3), (2, 1)) * 5)


class Line:
    def __init__(self):
        z, y, x, c = place()
        self.inner = (z == 1) | (z == 2)
        self.end = jnp.logical_not(self.inner)
        self.near = z + 1 - 2 * (z % 2)
        self.cross = (z + 2) % LINE
        self.far = LINE - 1 - z
        self.peers = [index_of(zz, y, x, c) for zz in (self.near, self.cross, self.far)]


class Reduce:
    def __init__(self, job, slot, g_ref, stage, sum1, got1, got2, got3, send, recv):
        self.color, self.unit, k = job
        self.g_ref = g_ref
        z, y, x, c = place()
        self.z = z
        self.late = self.color >= 2
        by_x = self.color % 2 == 0
        self.mine = y if by_x else x
        if by_x:
            group = ((y, 1 - x, c), (y, 1 - x, 1 - c), (y, x, 1 - c))
            side = index_of(z, 1 - y, x, c)
            part = lambda yy, xx, cc: stage.at[slot, :, :, xx, cc, k]
        else:
            group = ((1 - y, x, c), (1 - y, x, 1 - c), (y, x, 1 - c))
            side = index_of(z, y, 1 - x, c)
            part = lambda yy, xx, cc: stage.at[slot, :, yy, :, cc, k]
        self.own = part(y, x, c)
        self.sum1 = sum1.at[k]
        self.got1, self.got2, self.got3 = got1, got2, got3
        sems = Sems(send, recv)
        self.copies1 = [sems.copy(part(*who), got1.at[i], index_of(z, *who)) for i, who in enumerate(group)]
        line = Line()
        self.line = line
        if self.late:
            self.side = sems.copy(got2.at[0, 1 - self.mine], got3.at[0], side)
            self.from_z, self.to_z = got2, lambda zz: self.sum1.at[zz]
        else:
            self.side = sems.copy(self.sum1.at[:, 1 - self.mine], got2, side)
            self.from_z, self.to_z = got3, lambda zz: got2.at[zz]
        near, cross, far = line.peers
        self.near = sems.copy(self.to_z(line.near), self.from_z.at[0], near)
        self.cross = sems.copy(self.to_z(line.cross), self.from_z.at[1], cross)
        self.direct = sems.copy(self.to_z(line.far), self.from_z.at[2], far)
        self.relay = sems.copy(self.to_z(line.far), self.from_z.at[3], near)

    def start_line(self):
        self.near.start()

        @pl.when(self.line.inner)
        def _():
            self.direct.start()

        @pl.when(self.line.end)
        def _():
            self.relay.start()
            self.cross.start()

    def pass_on(self):
        @pl.when(self.line.inner)
        def _():
            self.relay.wait_recv()
            held, more = self.to_z(self.line.cross), self.from_z.at[3]
            if self.late:
                for side in range(2):
                    held[side] = held[side] + more[side]
            else:
                held[...] = held[...] + more[...]
            self.cross.start()

    def recv_line(self):
        self.near.wait_recv()
        self.cross.wait_recv()

        @pl.when(self.line.inner)
        def _():
            self.direct.wait_recv()

    def line_total(self, pick):
        total = pick(self.to_z(self.z)) + pick(self.from_z.at[0]) + pick(self.from_z.at[1])
        return total + jnp.where(self.line.inner, pick(self.from_z.at[2]), 0.0)

    def sent_line(self):
        self.near.wait_send()
        self.cross.wait_send()

        @pl.when(self.line.inner)
        def _():
            self.direct.wait_send()

        @pl.when(self.line.end)
        def _():
            self.relay.wait_send()

    def sent_sums(self):
        if self.late:
            self.sent_line()
        else:
            self.side.wait_send()

    def sent_rest(self):
        if self.late:
            self.side.wait_send()
        else:
            self.sent_line()

    def phase0(self):
        recv_all(self.copies1)

        def body(i, carry):
            zz, side = i // 2, i % 2
            total = self.own[zz, side].astype(jnp.float32)
            for k in range(len(self.copies1)):
                total = total + self.got1[k, zz, side].astype(jnp.float32)
            self.sum1[zz, side] = total
            return carry

        lax.fori_loop(0, 2 * LINE, body, 0)
        return self.start_line if self.late else self.side.start

    def phase1(self):
        if self.late:
            self.pass_on()
            return None
        self.side.wait_recv()

        def body(zz, carry):
            self.got2[zz] = self.got2[zz] + self.sum1[zz, self.mine]
            return carry

        lax.fori_loop(0, LINE, body, 0)
        return self.start_line

    def phase2(self):
        if not self.late:
            self.pass_on()
            return None
        self.recv_line()
        for side in range(2):
            self.got2[0, side] = self.line_total(lambda ref: ref[side])
        return self.side.start

    def phase3(self, begin, end, acc):
        if self.late:
            self.side.wait_recv()
            total = self.got2[0, self.mine] + self.got3[0]
        else:
            self.recv_line()
            total = self.line_total(lambda ref: ref[...])
        mean = total * (1.0 / DEVICES)
        self.g_ref[self.unit] = mean
        square = jnp.sum(mean * mean, axis=0)
        return acc + jnp.where((self.unit >= begin) & (self.unit < end), square, 0.0)


def start_all(copies):
    for copy in copies:
        copy.start()


def recv_all(copies):
    for copy in copies:
        copy.wait_recv()


def send_all(copies):
    for copy in copies:
        copy.wait_send()


def reduce_kernel(*args):
    tensors, (g_ref, n_ref, stage, sum1, norm_buf, in_sem, send_n, recv_n) = args[:TENSORS], args[TENSORS:TENSORS + 8]
    rest = args[TENSORS + 8:]
    z, y, x, c = place()
    me = lax.axis_index("dp")
    steps, sums = [], PHASE[2] + 1
    for t, jobs in enumerate(RS_STEPS):
        steps.append([])
        for job in jobs:
            steps[t].append(Reduce(job, t % DEPTH, g_ref, stage, sum1.at[t % sums], *rest[:5]))
            rest = rest[5:]
    count = len(steps)

    def start_in(t):
        if t < count:
            slot, first, units = t % DEPTH, steps[t][0].unit, len(steps[t])
            for r in range(DEVICES):
                zyx, core = divmod(r, 2)
                zy, xx = divmod(zyx, 2)
                zz, yy = divmod(zy, 2)
                runs = unit_runs(COVER_FIRST[r] + first, COVER_FIRST[r] + first + units)
                for src, dst in tile_copies(tensors, runs, stage.at[slot, zz, yy, xx, core]):
                    pltpu.make_async_copy(src, dst, in_sem.at[slot]).start()

    def start1(t):
        if t < count:
            part = stage.at[t % DEPTH, :, :, :, :, pl.ds(0, len(steps[t]))]
            pltpu.make_async_copy(part, part, in_sem.at[t % DEPTH]).wait()
            for k in range(3):
                for job in steps[t]:
                    job.copies1[k].start()

    for t in range(DEPTH):
        start_in(t)
    z_peers = Line().peers
    plane = [index_of(z, (y + k // LINE) % 2, (x + k // 2) % 2, (c + k) % 2) for k in range(1, SUB)]
    greet(plane + z_peers)
    first = first_unit(me)
    begin = first - jnp.minimum(first, END - COVER)
    end = begin + first_unit(me + 1) - first
    acc = jnp.zeros((SUB, LANES), jnp.float32)
    for t in range(AHEAD):
        start1(t)
    for t in range(count + PHASE[3]):
        start1(t + AHEAD)
        if t < count:
            if t >= sums:
                for job in steps[t - sums]:
                    job.sent_sums()
            start_all([Later(job.phase0()) for job in steps[t]])
            for job in steps[t]:
                send_all(job.copies1)
            start_in(t + DEPTH)
        if 0 <= t - PHASE[1] < count:
            start_all([Later(job.phase1()) for job in steps[t - PHASE[1]]])
        if 0 <= t - PHASE[2] < count:
            start_all([Later(job.phase2()) for job in steps[t - PHASE[2]]])
        if 0 <= t - PHASE[3]:
            for job in steps[t - PHASE[3]]:
                acc = job.phase3(begin, end, acc)

    sems = Sems(send_n, recv_n)
    sent, used = [], 0
    norm_buf[0] = acc
    for peers in (z_peers, plane):
        copies = [sems.copy(norm_buf.at[used], norm_buf.at[used + 1 + k], peer) for k, peer in enumerate(peers)]
        start_all(copies)
        recv_all(copies)
        sent += copies
        total = norm_buf[used]
        for k in range(len(peers)):
            total = total + norm_buf[used + 1 + k]
        used += 1 + len(peers)
        norm_buf[used] = total
    n_ref[0] = jnp.sum(norm_buf[used])

    send_all(sent)
    for t, jobs in enumerate(steps):
        for job in jobs:
            if t >= count - sums:
                job.sent_sums()
            job.sent_rest()


class Later:
    def __init__(self, action):
        self.action = action

    def start(self):
        if self.action is not None:
            self.action()


def reduce_scatter(tensors):
    dma = pltpu.SemaphoreType.DMA
    scratch = []
    most = max(len(jobs) for jobs in RS_STEPS)
    for color, unit, k in sum(RS_STEPS, []):
        late = color >= 2
        scratch += [
            pltpu.VMEM((3, LINE, 2) + TAIL, jnp.bfloat16),
            pltpu.VMEM(((LINE, 2) if late else (LINE,)) + TAIL, jnp.float32),
            pltpu.VMEM((1 if late else LINE,) + TAIL, jnp.float32),
            dma((OUTER,)),
            dma((OUTER,)),
        ]
    return pl.pallas_call(
        reduce_kernel,
        name="reduce_scatter",
        out_shape=[jax.ShapeDtypeStruct((COVER,) + TAIL, jnp.float32), jax.ShapeDtypeStruct((1,), jnp.float32)],
        in_specs=[ANY] * TENSORS,
        out_specs=[IN_VMEM, IN_SMEM],
        scratch_shapes=[
            pltpu.VMEM((DEPTH, LINE, 2, 2, 2, most) + TAIL, jnp.bfloat16),
            pltpu.VMEM((PHASE[2] + 1, most, LINE, 2) + TAIL, jnp.float32),
            pltpu.VMEM((NORM_SLOTS, SUB, LANES), jnp.float32),
            dma((DEPTH,)),
            dma((NORM_SLOTS,)),
            dma((NORM_SLOTS,)),
        ] + scratch,
        compiler_params=pltpu.CompilerParams(collective_id=0, has_side_effects=True, vmem_limit_bytes=BIG_VMEM),
    )(*tensors)


AG_STEPS = jobs_of(((0, 3), (2, 1), (2, 3)) * 4 + ((0, 3), (2, 1), (2,)))


class Gather:
    def __init__(self, job, a_ref, b_ref, send, recv):
        color, unit, _ = job
        u = pl.ds(unit, 1)
        z, y, x, c = place()
        y_peer, x_peer, c_peer = index_of(z, 1 - y, x, c), index_of(z, y, 1 - x, c), index_of(z, y, x, 1 - c)
        by_x = color % 2 == 0
        side, last = (y_peer, x_peer) if by_x else (x_peer, y_peer)
        sems = Sems(send, recv)
        here, row = b_ref.at[z, y, x, c, u], b_ref.at[:, y, x, c, u]
        half = b_ref.at[:, :, x, c, u] if by_x else b_ref.at[:, y, :, c, u]
        full = b_ref.at[:, :, :, c, u]
        self.late = color >= 2
        if self.late:
            at = lambda zz: b_ref.at[zz, :, x, c, u] if by_x else b_ref.at[zz, y, :, c, u]
            source, self.side = at(z), sems.copy(a_ref.at[u], here, side)
        else:
            at = lambda zz: b_ref.at[zz, y, x, c, u]
            source, self.side = a_ref.at[u], sems.copy(row, row, side)
        self.line = line = Line()
        self.near, self.cross, self.direct = (sems.copy(source, at(z), peer) for peer in line.peers)
        self.relay = sems.copy(at(line.cross), at(line.cross), line.peers[0])
        self.half, self.full = sems.copy(half, half, last), sems.copy(full, full, c_peer)

    def start_line(self):
        self.near.start()
        self.cross.start()

        @pl.when(self.line.inner)
        def _():
            self.direct.start()

    def pass_on(self):
        @pl.when(self.line.inner)
        def _():
            self.cross.wait_recv()
            self.relay.start()

    def recv_line(self):
        self.near.wait_recv()

        @pl.when(self.line.inner)
        def _():
            self.direct.wait_recv()

        @pl.when(self.line.end)
        def _():
            self.cross.wait_recv()
            self.relay.wait_recv()

    def phases(self):
        nothing = lambda: None
        if self.late:
            first = [(nothing, self.side.start), (self.side.wait_recv, self.start_line), (nothing, self.pass_on), (self.recv_line, self.half.start)]
        else:
            first = [(nothing, self.start_line), (nothing, self.pass_on), (self.recv_line, self.side.start), (self.side.wait_recv, self.half.start)]
        return first + [(self.half.wait_recv, self.full.start), (self.full.wait_recv, nothing)]

    def sent(self):
        for copy in (self.side, self.near, self.cross, self.half, self.full):
            copy.wait_send()

        @pl.when(self.line.inner)
        def _():
            self.direct.wait_send()
            self.relay.wait_send()


def gather_kernel(a_ref, b_ref, own_sem, *rest):
    z, y, x, c = place()
    greet(Line().peers + [index_of(z, 1 - y, x, c), index_of(z, y, 1 - x, c), index_of(z, y, x, 1 - c)])
    own = pltpu.make_async_copy(a_ref.at[pl.ds(0, GATHER)], b_ref.at[z, y, x, c], own_sem)
    own.start()
    steps, made = [], []
    for jobs in AG_STEPS:
        steps.append([])
        for job in jobs:
            made.append(Gather(job, a_ref, b_ref, *rest[:2]))
            steps[-1].append(made[-1].phases())
            rest = rest[2:]
    count, phases = len(steps), len(steps[0][0])

    def run(t, phase):
        if 0 <= t < count:
            for job in steps[t]:
                job[phase][0]()
                job[phase][1]()

    run(0, 0)
    own.wait()
    for t in range(count + phases):
        run(t + 1, 0)
        for phase in range(1, phases):
            run(t + 1 - phase, phase)
    for job in made:
        job.sent()


def all_gather(chunk):
    dma = pltpu.SemaphoreType.DMA
    out = pl.pallas_call(
        gather_kernel,
        name="all_gather",
        out_shape=jax.ShapeDtypeStruct((LINE, 2, 2, 2, GATHER) + TAIL, jnp.bfloat16),
        in_specs=[IN_VMEM],
        out_specs=ANY,
        scratch_shapes=[dma] + [dma((OUTER,))] * (2 * len(sum(AG_STEPS, []))),
        compiler_params=pltpu.CompilerParams(collective_id=1, has_side_effects=True, vmem_limit_bytes=BIG_VMEM),
    )(chunk)
    return out.reshape((DEVICES, GATHER) + TAIL)


def lanes(rows):
    return lax.broadcasted_iota(jnp.int32, (rows, LANES), 1)


def among(u, *starts):
    found = False
    for start in starts:
        stop = STARTS[STARTS.index(start) + 1]
        found = ((u >= start) & (u < stop)) | found
    return found


def rolled(value, shift):
    shift = shift % LANES
    return value if shift == 0 else pltpu.roll(value, shift, 1)


def turned(tiles):
    blank = [jnp.zeros((SUB, LANES), jnp.float32)] * (LANES // SUB - len(tiles))
    return jnp.concatenate(tiles + blank, axis=0).T


def narrow_blocks(width):
    step = LANES // width
    return [(col, min(step, HALF - col)) for col in range(0, HALF, step)]


def tile(ref, unit, index):
    return ref.at[pl.ds(pl.multiple_of(unit * ROWS + index * SUB, SUB), SUB), :]


def narrow_to_flat(in_ref, unit, flat, row, wide, width):
    per, step, lane = width // SUB, LANES // width, lanes(width)
    for col, count in narrow_blocks(width):
        wide[...] = turned([tile(in_ref, unit, HALF * r + col + e)[...] for e in range(count) for r in range(per)])
        for e in range(count):
            value = None
            for j in range(step):
                pick = rolled(wide[pl.ds(j, width, stride=step), :], width * (j - e))
                value = pick if value is None else jnp.where(lane >= width * j, pick, value)
            flat[pl.ds(row + width * (col + e), width), :] = value


def narrow_to_tiles(flat, row, out_ref, unit, wide, width):
    per, step, lane = width // SUB, LANES // width, lanes(width)
    for col, count in narrow_blocks(width):
        for j in range(step):
            value = None
            for e in range(count):
                pick = rolled(flat[pl.ds(row + width * (col + e), width), :], width * (e - j))
                value = pick if value is None else jnp.where(lane >= width * e, pick, value)
            wide[pl.ds(j, width, stride=step), :] = value
        back = wide[...].T
        for e in range(count):
            for r in range(per):
                at = width * e + SUB * r
                index = HALF * r + col + e
                out_ref[unit + index // TILES, index % TILES] = back[at:at + SUB].astype(jnp.bfloat16)


EDGE = ROWS - LANES


def unit_to_flat(in_ref, unit, flat, row, u, wide, tail):
    @pl.when(among(u, EMBED, OUT, DOWN))
    def _():
        for e in range(SUB):
            flat[pl.ds(row + TILES * e, TILES), :] = in_ref[pl.ds(row + e, TILES, stride=SUB), :]

    @pl.when(among(u, NORMS))
    def _():
        flat[pl.ds(row, ROWS), :] = in_ref[pl.ds(row, ROWS), :]

    @pl.when(among(u, K, V))
    def _():
        narrow_to_flat(in_ref, unit, flat, row, wide, EDGE)

    @pl.when(among(u, GATE, UP))
    def _():
        wide[...] = turned([tile(in_ref, unit, t)[...] for t in range(LANES // SUB)])
        tail[:, 0:EDGE] = jnp.concatenate([tile(in_ref, unit, t)[...] for t in range(LANES // SUB, TILES)], axis=0).T
        lane = lanes(EDGE)
        before = None
        for j in range(SUB):
            head = rolled(wide[pl.ds(j, EDGE, stride=SUB), :], EDGE * j)
            rest = rolled(tail[pl.ds(j, EDGE, stride=SUB), :], EDGE * j)
            flat[pl.ds(row + j, EDGE, stride=HALF), :] = head if before is None else jnp.where(lane < EDGE * j, before, head)
            before = jnp.where((lane >= EDGE * j) & (lane < EDGE * (j + 1)), rest, head)
        flat[pl.ds(row + SUB, EDGE, stride=HALF), :] = before


def unit_to_tiles(flat, row, out_ref, unit, u, wide, tail):
    @pl.when(among(u, EMBED, OUT, DOWN))
    def _():
        for t in range(TILES):
            out_ref[unit, t] = flat[pl.ds(row + t, SUB, stride=TILES), :].astype(jnp.bfloat16)

    @pl.when(among(u, NORMS))
    def _():
        out_ref[unit] = flat[pl.ds(row, ROWS), :].reshape(TAIL).astype(jnp.bfloat16)

    @pl.when(among(u, K, V))
    def _():
        narrow_to_tiles(flat, row, out_ref, unit, wide, EDGE)

    @pl.when(among(u, GATE, UP))
    def _():
        lane = lanes(EDGE)
        for j in range(SUB):
            here = flat[pl.ds(row + j, EDGE, stride=HALF), :]
            after = flat[pl.ds(row + j + 1, EDGE, stride=HALF), :]
            wide[pl.ds(j, EDGE, stride=SUB), :] = rolled(jnp.where(lane >= EDGE * j, here, after), -EDGE * j)
            tail[pl.ds(j, EDGE, stride=SUB), :] = rolled(after, -EDGE * j)
        out_ref[unit, pl.ds(0, LANES // SUB)] = wide[...].T.reshape(LANES // SUB, SUB, LANES).astype(jnp.bfloat16)
        out_ref[unit, pl.ds(LANES // SUB, 2)] = tail[:, 0:EDGE].T.reshape(2, SUB, LANES).astype(jnp.bfloat16)


def local_place():
    me = lax.axis_index("dp")
    return me, first_unit(me)


def blocks_of(rows, block, body):
    def step(i, carry):
        body(pl.multiple_of(i * block, SUB))
        return carry

    lax.fori_loop(0, rows // block, step, 0)


def to_flat_kernel(in_ref, out_ref, flat, wide, tail):
    me, first = local_place()
    first = jnp.minimum(first, END - COVER)
    offset = me * SHARD - first * UNIT

    def pair(i, carry):
        unit = 2 * i
        u = first + unit

        @pl.when(among(u, Q))
        def _():
            narrow_to_flat(in_ref, unit, flat, unit * ROWS, wide, 2 * EDGE)

        for j in range(2):
            unit_to_flat(in_ref, unit + j, flat, (unit + j) * ROWS, u + j, wide, tail)
        return carry

    lax.fori_loop(0, COVER // 2, pair, 0)
    flat[pl.ds(FLAT_ROWS, SUB), :] = jnp.zeros((SUB, LANES), jnp.float32)
    row, left = offset // LANES, offset % LANES
    lane = lanes(OWN_BLOCK)
    turn = (LANES - left) % LANES

    def move(k):
        here = flat[pl.ds(row + k, OWN_BLOCK), :]
        after = flat[pl.ds(row + k + 1, OWN_BLOCK), :]
        out_ref[pl.ds(k, OWN_BLOCK), :] = pltpu.roll(jnp.where(lane >= left, here, after), turn, 1)

    blocks_of(OWN_ROWS, OWN_BLOCK, move)


def to_flat(tiles):
    square = pltpu.VMEM((LANES, LANES), jnp.float32)
    return pl.pallas_call(
        to_flat_kernel,
        name="to_flat",
        out_shape=jax.ShapeDtypeStruct((OWN_ROWS, LANES), jnp.float32),
        in_specs=[IN_VMEM],
        out_specs=IN_VMEM,
        scratch_shapes=[pltpu.VMEM((FLAT_ROWS + SUB, LANES), jnp.float32), square, square],
    )(tiles.reshape(FLAT_ROWS, LANES))


def to_tiles_kernel(before_ref, in_ref, out_ref, joined, flat, wide, tail):
    me, first = local_place()
    offset = me * SHARD - first * UNIT
    row, left = offset // LANES, offset % LANES
    lane = lanes(ROWS)

    def fill(ref, base, block):
        def move(k):
            joined[pl.ds(base + k, block), :] = pltpu.roll(ref[pl.ds(k, block), :], left, 1)
        return move

    blocks_of(HALO, ROWS, fill(before_ref, 0, ROWS))
    blocks_of(OWN_ROWS, OWN_BLOCK, fill(in_ref, HALO, OWN_BLOCK))
    joined[pl.ds(HALO + OWN_ROWS, FLAT_ROWS - OWN_ROWS), :] = jnp.zeros((FLAT_ROWS - OWN_ROWS, LANES), jnp.float32)

    def align(k):
        here = joined[pl.ds(HALO - row + k, ROWS), :]
        above = joined[pl.ds(HALO - 1 - row + k, ROWS), :]
        flat[pl.ds(k, ROWS), :] = jnp.where(lane >= left, here, above)

    blocks_of(FLAT_ROWS, ROWS, align)

    def pair(i, carry):
        unit = 2 * i
        u = first + unit

        @pl.when(among(u, Q))
        def _():
            narrow_to_tiles(flat, unit * ROWS, out_ref, unit, wide, 2 * EDGE)

        for j in range(2):
            unit_to_tiles(flat, (unit + j) * ROWS, out_ref, unit + j, u + j, wide, tail)
        return carry

    lax.fori_loop(0, COVER // 2, pair, 0)


def to_tiles(before, share):
    square = pltpu.VMEM((LANES, LANES), jnp.float32)
    return pl.pallas_call(
        to_tiles_kernel,
        name="to_tiles",
        out_shape=jax.ShapeDtypeStruct((COVER,) + TAIL, jnp.bfloat16),
        in_specs=[IN_VMEM, IN_VMEM],
        out_specs=IN_VMEM,
        scratch_shapes=[pltpu.VMEM((HALO + FLAT_ROWS, LANES), jnp.float32), pltpu.VMEM((FLAT_ROWS, LANES), jnp.float32), square, square],
    )(before, share)


def adam_step(grad_part, first_part, second_part, master_part, hyper_params, clip_scale, keep_decay):
    learn_rate, beta_one, beta_two, weight_decay = (hyper_params[k] for k in range(4))
    rest, warm = 1.0 - hyper_params, 1.0 - hyper_params ** ADAM_STEP
    rest_one, rest_two, warm_one, warm_two = rest[1], rest[2], warm[1], warm[2]
    clipped = grad_part * clip_scale
    moment_one = beta_one * first_part + rest_one * clipped
    moment_two = beta_two * second_part + rest_two * (clipped * clipped)
    m_hat = moment_one / warm_one
    v_hat = moment_two / warm_two
    direction = m_hat / (jnp.sqrt(v_hat) + ADAM_EPS) + jnp.where(keep_decay, weight_decay * master_part, 0.0)
    new_master = master_part - learn_rate * direction
    return moment_one, moment_two, new_master


def row_tiles(mat):
    return mat.reshape(-1, SUB, TILES, LANES).transpose(0, 2, 1, 3)


def from_row_tiles(tiles):
    return tiles.transpose(0, 2, 1, 3).reshape(-1, WIDTH)


def solution(mesh):
    def local_update(*arrays):
        grads, (first_part, second_part, master_part, hyper_params) = arrays[:-4], arrays[-4:]
        me = lax.axis_index("dp")

        def tiles_of(tensor):
            arr, kind = grads[tensor], STARTS[tensor]
            if kind in (EMBED, OUT, DOWN):
                return row_tiles(arr.reshape(-1, WIDTH))
            width = arr.shape[-1]
            tiles = row_tiles(arr.reshape(LAYERS, WIDTH, width).transpose(0, 2, 1).reshape(-1, WIDTH))
            return tiles.reshape((LAYERS, width // SUB) + TAIL)

        tensors = [tiles_of(k) for k in range(TENSORS - 1)]
        blank = jnp.zeros(((END - NORMS) * UNIT - NORM_LEN,), jnp.bfloat16)
        small = jnp.concatenate([arr.reshape(-1) for arr in grads[TENSORS - 1:]] + [blank])
        tensors.append(small.reshape((END - NORMS,) + TAIL))
        grad_tiles, squares = reduce_scatter(tensors)
        clip_scale = jnp.minimum(1.0, hyper_params[4] / (jnp.sqrt(squares[0]) + CLIP_EPS))
        grad_part = to_flat(grad_tiles).reshape(-1)[:SHARD]
        keep_decay = me * SHARD + lax.broadcasted_iota(jnp.int32, (SHARD,), 0) < SHARD * DEVICES - NORM_LEN
        moment_one, moment_two, new_master = adam_step(grad_part, first_part, second_part, master_part, hyper_params, clip_scale, keep_decay)
        before = lax.ppermute(new_master[SHARD - HALO * LANES:], "dp", [(r, r + 1) for r in range(DEVICES - 1)])
        padded = jnp.pad(new_master, (0, OWN_ROWS * LANES - SHARD))
        chunk = to_tiles(before.reshape(HALO, LANES), padded.reshape(OWN_ROWS, LANES))
        outs = unpack(all_gather(chunk), [t.shape for t in tensors])

        def tensor_of(tensor):
            tiles, dims = outs[tensor], grads[tensor].shape[1:]
            if STARTS[tensor] in (EMBED, OUT, DOWN):
                return from_row_tiles(tiles).reshape(dims)
            mat = from_row_tiles(tiles.reshape((-1,) + TAIL))
            return mat.reshape(LAYERS, dims[-1], WIDTH).transpose(0, 2, 1)

        results = [tensor_of(k) for k in range(TENSORS - 1)]
        flat_small, start = outs[-1].reshape(-1), 0
        for arr in grads[TENSORS - 1:]:
            size = math.prod(arr.shape)
            results.append(flat_small[start:start + size].reshape(arr.shape[1:]))
            start += size
        return tuple(results) + (moment_one, moment_two, new_master)

    in_specs = tuple([P("dp")] * 13 + [P()])
    out_specs = tuple([P()] * 10 + [P("dp"), P("dp"), P("dp")])
    return jax.shard_map(local_update, mesh=mesh, in_specs=in_specs, out_specs=out_specs, check_vma=False)
```
